32 devices in a mesh: gx: 4 (over y, core), gy: 2 (over x), gz: 4 (over z).
Axes of the slice: x: 2, y: 2, z: 4, core: 2. Of those that a mesh axis runs over, the one named last changes fastest.
Arguments:
- density: float32 [32, 32, 512], P('gx', 'gy', 'gz'), may hold values from 0.7 to 1.6
- momentum: float32 [32, 32, 512], P('gx', 'gy', 'gz'), may hold values from -7 to 7
- hydrogen: float32 [32, 32, 512], P('gx', 'gy', 'gz'), may hold values from 0.05 to 1.2
- forced_modes: int32 [96, 3], replicated, may hold values from -3 to 3, as said below
Outputs:
- density_rate: float32 [32, 32, 512], P('gx', 'gy', 'gz')
- momentum_rate: float32 [32, 32, 512], P('gx', 'gy', 'gz')
- hydrogen_rate: float32 [32, 32, 512], P('gx', 'gy', 'gz')
The draws below stay inside these ranges and needn't reach their ends.
Inputs may be any that keep to these rules, and one draw needn't show every extreme that they name: `forced_modes`: each row is a wave vector (kx, ky, kz) with 1 <= kx^2 + ky^2 + kz^2 <= 9; the 96 rows are distinct.
All inputs are finite; a program needn't handle non-finite values.
Results may differ from the reference program's by a relative error of at most 0.0003.
Values sent between devices are 32-bit elements; how exact they have to be, the bound alone decides.
A program may use at most 64 MiB of HBM per device.

```python
import jax
import jax.numpy as jnp
import numpy as np
from jax import lax

KMAX = 3
MODES = 96
NX = 32
NY = 32
NZ = 512


def draw_momentum(key, part):
    keys = jax.random.split(key, 6)
    noise = jnp.clip(0.35 * jax.random.normal(keys[0], (NX, NY, NZ), jnp.float32), -1.4, 1.4)
    amp_low = 0.4
    amp_high = 1.0
    total = noise
    for term in range(4):
        sub = jax.random.split(keys[term + 1], 3)
        wavevec = jax.random.randint(sub[0], (3,), 0, 2).astype(jnp.float32)
        phases = jax.random.uniform(sub[1], (3,), jnp.float32, -jnp.pi, jnp.pi)
        amplitude = jax.random.uniform(sub[2], (), jnp.float32, amp_low, amp_high)
        wave_x = jnp.cos(2.0 * jnp.pi * wavevec[0] * jnp.arange(NX, dtype=jnp.float32) / NX + phases[0])
        wave_y = jnp.cos(2.0 * jnp.pi * wavevec[1] * jnp.arange(NY, dtype=jnp.float32) / NY + phases[1])
        wave_z = jnp.cos(2.0 * jnp.pi * wavevec[2] * jnp.arange(NZ, dtype=jnp.float32) / NZ + phases[2])
        total = total + amplitude * wave_x[:, None, None] * wave_y[None, :, None] * wave_z[None, None, :]
    return total.astype(jnp.float32)


def wave_sheet(key, rows, cols, theta_low, theta_high):
    keys = jax.random.split(key, 3)
    theta = jax.random.uniform(keys[0], (3,), jnp.float32, theta_low, theta_high)
    drift = jax.random.uniform(keys[1], (3,), jnp.float32, -0.2, 0.2)
    phase = jax.random.uniform(keys[2], (3,), jnp.float32, -jnp.pi, jnp.pi)
    across = jnp.arange(rows, dtype=jnp.float32)[:, None]
    along = jnp.arange(cols, dtype=jnp.float32)[None, :]
    total = jnp.zeros((rows, cols), jnp.float32)
    for term in range(3):
        total = total + 0.09 * jnp.cos(theta[term] * along + drift[term] * across + phase[term])
    return total


def draw_hydrogen(key, part):
    keys = jax.random.split(key, 3)
    sheet_y = wave_sheet(keys[0], NX, NY, 0.5, 1.05)
    sheet_z = wave_sheet(keys[1], NX, NZ, 0.5, 1.05)
    rough = jnp.clip(0.02 * jax.random.normal(keys[2], (NX, NY, NZ), jnp.float32), -0.045, 0.045)
    smooth = 0.6 + sheet_y[:, :, None] + sheet_z[:, None, :]
    return (smooth * (1.0 + rough)).astype(jnp.float32)


def draw_forced_modes(key, part):
    grid = np.arange(-3, 4)
    triples = np.stack(np.meshgrid(grid, grid, grid, indexing='ij'), -1).reshape(-1, 3)
    radius = np.sum(triples * triples, axis=1)
    valid = triples[(radius >= 1) & (radius <= 9)].astype(np.int32)
    chosen = jax.random.permutation(key, valid.shape[0])[:MODES]
    return jnp.asarray(valid)[chosen].astype(jnp.int32)


def steps_of(rng, shape, pieces, smallest, high):
    gain = 1.0
    for axis_at, shards_of in pieces:
        heights = jax.random.uniform(jax.random.fold_in(jax.random.fold_in(rng, 6), axis_at), (shards_of,), jnp.float32, smallest / len(pieces), high / len(pieces))
        gain = gain * jnp.repeat(jnp.exp(heights), shape[axis_at] // shards_of).reshape((-1,) + (1,) * (len(shape) - 1 - axis_at))
    return gain


def setup_inputs(seed: int = 0) -> dict:
    streams_of = jax.random.split(jax.random.key(seed), 5)
    density = jnp.clip(0.7 + 0.90000004 * jax.random.uniform(streams_of[0], (NX, NY, NZ), jnp.float32) ** steps_of(streams_of[0], (NX, NY, NZ), ((0, 4), (1, 2), (2, 4)), -0.2, 0.2), 0.7, 1.6)
    momentum = draw_momentum(jax.random.fold_in(streams_of[4], 71), 0)
    hydrogen = draw_hydrogen(jax.random.fold_in(streams_of[4], 71), 0)
    forced_modes = draw_forced_modes(jax.random.fold_in(streams_of[4], 71), 0)
    return dict(density=density, momentum=momentum, hydrogen=hydrogen, forced_modes=forced_modes)


FIRST_COEFFS = (0.8, -0.2, 4.0 / 105.0, -1.0 / 280.0)
SECOND_COEFFS = (1.6, -0.2, 8.0 / 315.0, -1.0 / 560.0)
CENTRE_COEFF = -205.0 / 72.0
VISCOSITY = 0.3
DIFFUSIVITY = 1.5
FORCE_POWER = 0.3
ENERGY_EPS = 1e-6
ACTIVATION = 2.0
HIGHEST = lax.Precision.HIGHEST


def first_diff(field, axis):
    total = jnp.zeros_like(field)
    for offset, weight in enumerate(FIRST_COEFFS, 1):
        total = total + weight * (jnp.roll(field, -offset, axis) - jnp.roll(field, offset, axis))
    return total


def second_diff(field, axis):
    total = CENTRE_COEFF * field
    for offset, weight in enumerate(SECOND_COEFFS, 1):
        total = total + weight * (jnp.roll(field, -offset, axis) + jnp.roll(field, offset, axis))
    return total


def wave_tables(start, local, total):
    position = start + jnp.arange(local, dtype=jnp.int32)
    wavenum = jnp.arange(-KMAX, KMAX + 1, dtype=jnp.int32)
    phase = (wavenum[:, None] * position[None, :]) % total
    angle = (2.0 * jnp.pi / total) * phase.astype(jnp.float32)
    return jnp.cos(angle), jnp.sin(angle)


def reference(density, momentum, hydrogen, forced_modes):
    size_x, size_y, size_z = density.shape
    velocity = momentum / density
    cos_x, sin_x = wave_tables(0, size_x, size_x)
    cos_y, sin_y = wave_tables(0, size_y, size_y)
    cos_z, sin_z = wave_tables(0, size_z, size_z)
    flat = velocity.reshape(size_x * size_y, size_z)
    part_re = jnp.dot(cos_z, flat.T, precision=HIGHEST).reshape(-1, size_x, size_y)
    part_im = jnp.dot(sin_z, flat.T, precision=HIGHEST).reshape(-1, size_x, size_y)
    mid_re = jnp.einsum('axy,by->abx', part_re, cos_y, precision=HIGHEST) - jnp.einsum('axy,by->abx', part_im, sin_y, precision=HIGHEST)
    mid_im = jnp.einsum('axy,by->abx', part_re, sin_y, precision=HIGHEST) + jnp.einsum('axy,by->abx', part_im, cos_y, precision=HIGHEST)
    cube_re = jnp.einsum('abx,cx->cba', mid_re, cos_x, precision=HIGHEST) - jnp.einsum('abx,cx->cba', mid_im, sin_x, precision=HIGHEST)
    cube_im = jnp.einsum('abx,cx->cba', mid_re, sin_x, precision=HIGHEST) + jnp.einsum('abx,cx->cba', mid_im, cos_x, precision=HIGHEST)
    width = 2 * KMAX + 1
    code = (forced_modes[:, 0] + KMAX) * width * width + (forced_modes[:, 1] + KMAX) * width + (forced_modes[:, 2] + KMAX)
    selector = (code[:, None] == jnp.arange(width ** 3, dtype=jnp.int32)[None, :]).astype(jnp.float32)
    ncell = float(size_x * size_y * size_z)
    coef_cos = jnp.dot(selector, cube_re.reshape(-1), precision=HIGHEST) / ncell
    coef_sin = jnp.dot(selector, cube_im.reshape(-1), precision=HIGHEST) / ncell
    energy = jnp.sum(coef_cos * coef_cos + coef_sin * coef_sin)
    spec_re = jnp.dot(selector.T, coef_cos, precision=HIGHEST).reshape(width, width, width)
    spec_im = -jnp.dot(selector.T, coef_sin, precision=HIGHEST).reshape(width, width, width)
    step_re = jnp.einsum('abc,ax->xbc', spec_re, cos_x, precision=HIGHEST) - jnp.einsum('abc,ax->xbc', spec_im, sin_x, precision=HIGHEST)
    step_im = jnp.einsum('abc,ax->xbc', spec_re, sin_x, precision=HIGHEST) + jnp.einsum('abc,ax->xbc', spec_im, cos_x, precision=HIGHEST)
    plane_re = jnp.einsum('xbc,by->xyc', step_re, cos_y, precision=HIGHEST) - jnp.einsum('xbc,by->xyc', step_im, sin_y, precision=HIGHEST)
    plane_im = jnp.einsum('xbc,by->xyc', step_re, sin_y, precision=HIGHEST) + jnp.einsum('xbc,by->xyc', step_im, cos_y, precision=HIGHEST)
    low = 2.0 * (jnp.dot(plane_re.reshape(-1, width), cos_z, precision=HIGHEST) - jnp.dot(plane_im.reshape(-1, width), sin_z, precision=HIGHEST))
    force = FORCE_POWER * low.reshape(size_x, size_y, size_z) / (energy + ENERGY_EPS)
    density_rate = -first_diff(momentum, 0)
    lap_mom = second_diff(momentum, 0) + second_diff(momentum, 1) + second_diff(momentum, 2)
    lap_fuel = second_diff(hydrogen, 0) + second_diff(hydrogen, 1) + second_diff(hydrogen, 2)
    momentum_rate = -first_diff(momentum * velocity + density, 0) + VISCOSITY * lap_mom + density * force
    hydrogen_rate = -first_diff(hydrogen * velocity, 0) + DIFFUSIVITY * lap_fuel - hydrogen * jnp.exp(-ACTIVATION * hydrogen / density)
    return density_rate, momentum_rate, hydrogen_rate
```

```python
import functools
import math

import jax
import jax.numpy as jnp
import numpy as np
from jax import lax
from jax.experimental import pallas as pl
from jax.experimental.pallas import tpu as pltpu
from jax.sharding import PartitionSpec as P

KMAX = 3
WIDTH = 2 * KMAX + 1
HALF = 64
REACH = 4

FIRST_COEFFS = (0.8, -0.2, 4.0 / 105.0, -1.0 / 280.0)
SECOND_COEFFS = (1.6, -0.2, 8.0 / 315.0, -1.0 / 560.0)
CENTRE_COEFF = -205.0 / 72.0
VISCOSITY = 0.3
DIFFUSIVITY = 1.5
FORCE_POWER = 0.3
ENERGY_EPS = 1e-06
ACTIVATION = 2.0
HIGHEST = lax.Precision.HIGHEST
MESH = pl.DeviceIdType.MESH


def tables(local, full):
    size_x, size_y, size_z = local
    full_x, full_y, full_z = full
    k = np.arange(-KMAX, KMAX + 1)
    ang_z = 2.0 * np.pi * (k[:, None] * np.arange(size_z)[None, :]) / full_z
    trig_z = np.zeros((16, size_z))
    trig_z[:WIDTH] = np.cos(ang_z)
    trig_z[8 : 8 + WIDTH] = np.sin(ang_z)
    ax = k[:, None] * np.arange(size_x)[None, :] / full_x
    ay = k[:, None] * np.arange(size_y)[None, :] / full_y
    ang = 2.0 * np.pi * (ax[:, None, :, None] + ay[None, :, None, :])
    ang = ang.reshape(WIDTH * WIDTH, size_x * size_y)
    trig_xy = np.zeros((2 * HALF, size_x * size_y))
    trig_xy[: WIDTH * WIDTH] = np.cos(ang)
    trig_xy[HALF : HALF + WIDTH * WIDTH] = np.sin(ang)
    edge = np.zeros((8, size_z))
    for j in range(REACH):
        edge[j, j] = 1.0
        edge[REACH + j, size_z - REACH + j] = 1.0
    band = np.zeros((size_z, size_z))
    halo = np.zeros((16, size_z))
    for z in range(size_z):
        band[z, z] = 3.0 * CENTRE_COEFF
        for offset, weight in enumerate(SECOND_COEFFS, 1):
            for q in (z - offset, z + offset):
                if 0 <= q < size_z:
                    band[q, z] = weight
                elif q < 0:
                    halo[8 + q, z] = weight
                else:
                    halo[8 + q - size_z, z] = weight
    early = np.concatenate([trig_z, edge, trig_xy], 0).astype(np.float32)
    late = np.concatenate([halo, band], 0).astype(np.float32)
    return early, late


def dot_nt(a, b):
    return lax.dot_general(a, b, (((1,), (1,)), ((), ())), precision=HIGHEST, preferred_element_type=jnp.float32)


def dot_nn(a, b):
    return lax.dot_general(a, b, (((1,), (0,)), ((), ())), precision=HIGHEST, preferred_element_type=jnp.float32)


def dot_tn(a, b):
    return lax.dot_general(a, b, (((0,), (0,)), ((), ())), precision=HIGHEST, preferred_element_type=jnp.float32)


def group_offsets(sizes, axes):
    offsets = [{}]
    for axis in axes:
        offsets = [{**o, axis: s} for o in offsets for s in range(sizes[axis])]
    return [o for o in offsets if any(o.values())]


def tree_sum(parts):
    parts = list(parts)
    while len(parts) > 1:
        parts = [sum(parts[i : i + 2][1:], parts[i]) for i in range(0, len(parts), 2)]
    return parts[0]


def plan(sizes):
    if sizes["gx"] * sizes["gy"] <= 16:
        stages = [("gz",), ("gx", "gy")]
    else:
        stages = [("gz",), ("gx",), ("gy",)]
    return [group_offsets(sizes, s) for s in stages]


def kernel(sizes, local, dens_hbm, mom_hbm, fuel_hbm, modes_hbm, early_hbm, late_hbm,
           drate_hbm, mrate_hbm, hrate_hbm,
           f, modes, early, late, edges, sides, ypack, zpack, ztile, stage_own, stage_got, outs,
           load_sem, store_sem, halo_send, halo_recv, stage_send, stage_recv):
    size_x, size_y, size_z = local
    rows = size_x * size_y
    me = {a: lax.axis_index(a) for a in sizes}
    stages = plan(sizes)

    def at(offset):
        return {a: lax.rem(me[a] + o, sizes[a]) for a, o in offset.items()}

    own = pl.ds(REACH, size_x)
    loads = [
        pltpu.make_async_copy(src, dst, load_sem.at[i])
        for i, (src, dst) in enumerate([
            (dens_hbm, f.at[0, own]), (mom_hbm, f.at[1, own]), (early_hbm, early),
            (fuel_hbm, f.at[2, own]), (modes_hbm, modes), (late_hbm, late),
        ])
    ]
    for copy in loads:
        copy.start()
    barrier = pltpu.get_barrier_semaphore()
    partners = [o for group in stages for o in group]
    for offset in partners:
        pl.semaphore_signal(barrier, inc=1, device_id=at(offset), device_id_type=MESH)

    row = lax.broadcasted_iota(jnp.int32, (8, 2 * HALF), 0)
    lane = lax.broadcasted_iota(jnp.int32, (8, 2 * HALF), 1)
    pair = lax.rem(lane, HALF)
    kx = lax.div(pair, WIDTH)
    ky = pair - kx * WIDTH
    turn = jnp.zeros((8, 2 * HALF), jnp.float32)
    for k, axis, size in ((kx, "gx", size_x), (ky, "gy", size_y), (row, "gz", size_z)):
        count = (k - KMAX).astype(jnp.float32) * me[axis].astype(jnp.float32)
        part = count / sizes[axis]
        turn = turn + (part - jnp.floor(part))
    turn = turn - jnp.floor(turn + 0.5)
    cos_p = jnp.cos(2.0 * math.pi * turn)
    sin_p = jnp.sin(2.0 * math.pi * turn)
    sign = jnp.where(lane < HALF, -1.0, 1.0)
    sin_p = sign * sin_p

    loads[0].wait()
    loads[1].wait()
    loads[2].wait()
    flat = lambda i: f[i, own].reshape(rows, size_z)
    vel = flat(1) / flat(0)
    trig_z = early[0:16]
    trig_xy = early[24 : 24 + 2 * HALF]
    grid = dot_nt(dot_nt(trig_z, vel), trig_xy)
    cube = grid[0:8] + sign * pltpu.roll(grid[8:16], HALF, 1)
    cube = cos_p * cube + sin_p * pltpu.roll(cube, HALF, 1)
    stage_own[0] = cube

    def send_stage(s):
        base = sum(len(g) for g in stages[:s])
        copies = []
        for i, offset in enumerate(stages[s]):
            copy = pltpu.make_async_remote_copy(
                src_ref=stage_own.at[s], dst_ref=stage_got.at[base + i],
                send_sem=stage_send.at[base + i], recv_sem=stage_recv.at[base + i],
                device_id=at(offset), device_id_type=MESH)
            copy.start()
            copies.append(copy)
        return copies

    def sum_stage(s, copies):
        base = sum(len(g) for g in stages[:s])
        for copy in copies:
            copy.wait_recv()
        return tree_sum([stage_own[s]] + [stage_got[base + i] for i in range(len(copies))])

    pl.semaphore_wait(barrier, len(partners))
    pending = send_stage(0)
    started = list(pending)
    loads[3].wait()

    def send(src, dst, slot, axis, step):
        copy = pltpu.make_async_remote_copy(
            src_ref=src, dst_ref=dst, send_sem=halo_send.at[slot], recv_sem=halo_recv.at[slot],
            device_id=at({axis: step % sizes[axis]}), device_id_type=MESH)
        copy.start()
        return copy

    halos_x = [
        send(f.at[:, pl.ds(size_x, REACH)], f.at[:, pl.ds(0, REACH)], 0, "gx", 1),
        send(f.at[:, pl.ds(REACH, REACH)], f.at[:, pl.ds(size_x + REACH, REACH)], 1, "gx", -1),
    ]
    for i in range(2):
        ypack[i, :, 0:REACH] = f[1 + i, own, 0:REACH]
        ypack[i, :, REACH : 2 * REACH] = f[1 + i, own, size_y - REACH : size_y]
        zpack[i] = dot_nt(early[16:24], flat(1 + i))
    halos_y = [send(ypack, sides.at[0], 2, "gy", 1)]
    if sizes["gy"] > 2:
        halos_y.append(send(ypack, sides.at[1], 3, "gy", -1))
    halos_z = [send(zpack, ztile.at[0], 4, "gz", 1), send(zpack, ztile.at[1], 5, "gz", -1)]

    loads[4].wait()
    hit_z = lax.broadcasted_iota(jnp.int32, (8, modes.shape[1]), 0) == modes[2:3] + KMAX
    code = (modes[0:1] + KMAX) * WIDTH + modes[1:2] + KMAX
    hit_xy = lax.rem(lax.broadcasted_iota(jnp.int32, (2 * HALF, modes.shape[1]), 0), HALF) == code
    chosen = dot_nt(hit_z.astype(jnp.float32), hit_xy.astype(jnp.float32))

    loads[5].wait()
    lap = [dot_nn(flat(1 + i), late[16 : 16 + size_z]).reshape(size_x, size_y, size_z) for i in range(2)]
    outs[1] = lap[0]
    outs[2] = lap[1]

    for s in range(1, len(stages)):
        stage_own[s] = sum_stage(s - 1, pending)
        pending = send_stage(s)
        started += pending

    for copy in halos_z:
        copy.wait_recv()
    for copy in halos_y:
        copy.wait_recv()
    for i in range(2):
        tile = jnp.concatenate([ztile[0, i], ztile[1, i]], 0)
        edges[i, :, 0:8] = sides[0, i]
        edges[i, :, 8 : 8 + size_y] = f[1 + i, own]
        edges[i, :, 8 + size_y : 16 + size_y] = sides[1 if sizes["gy"] > 2 else 0, i]
        total = outs[1 + i] + dot_tn(tile, late[0:16]).reshape(size_x, size_y, size_z)
        for offset, weight in enumerate(SECOND_COEFFS, 1):
            total = total + weight * (
                edges[i, :, 8 + offset : 8 + offset + size_y] + edges[i, :, 8 - offset : 8 - offset + size_y])
        outs[1 + i] = total

    for copy in halos_x:
        copy.wait_recv()
    def planes(x, offset):
        return x[REACH + offset : REACH + offset + size_x]

    def first_diff(x):
        total = None
        for offset, weight in enumerate(FIRST_COEFFS, 1):
            term = weight * (planes(x, offset) - planes(x, -offset))
            total = term if total is None else total + term
        return total

    def second_diff(x):
        return tree_sum([w * (planes(x, o) + planes(x, -o)) for o, w in enumerate(SECOND_COEFFS, 1)])

    mom = f[1]
    dens = f[0]
    fuel = f[2]
    vel_pad = mom / dens
    outs[0] = -first_diff(mom)
    stores = [pltpu.make_async_copy(outs.at[0], drate_hbm, store_sem.at[0])]
    stores[0].start()
    mid_fuel = planes(fuel, 0)
    outs[2] = (DIFFUSIVITY * (outs[2] + second_diff(fuel)) - first_diff(fuel * vel_pad)
               - mid_fuel * jnp.exp(-ACTIVATION * mid_fuel / planes(dens, 0)))
    stores.append(pltpu.make_async_copy(outs.at[2], hrate_hbm, store_sem.at[1]))
    stores[1].start()
    outs[1] = VISCOSITY * (outs[1] + second_diff(mom)) - first_diff(mom * vel_pad + dens)

    ncell = float(rows * size_z * math.prod(sizes.values()))
    cube = sum_stage(len(stages) - 1, pending)
    coef = chosen * cube / ncell
    energy = jnp.sum(jnp.sum(coef * coef, axis=1, keepdims=True), axis=0, keepdims=True)
    scale = 2.0 * FORCE_POWER / (energy + ENERGY_EPS)
    local_coef = cos_p * coef - sin_p * pltpu.roll(coef, HALF, 1)
    both = jnp.concatenate([local_coef, -sign * pltpu.roll(local_coef, HALF, 1)], 0)
    low = dot_tn(dot_nn(both, trig_xy), trig_z).reshape(size_x, size_y, size_z)
    outs[1] = outs[1] + f[0, own] * (low * scale.reshape(1, 1, 1))
    stores.append(pltpu.make_async_copy(outs.at[1], mrate_hbm, store_sem.at[2]))
    stores[2].start()
    for copy in started + halos_x + halos_y + halos_z:
        copy.wait_send()
    for copy in stores:
        copy.wait()


def solution(mesh):
    sizes = {a: mesh.shape[a] for a in ("gx", "gy", "gz")}

    def per_device(density, momentum, hydrogen, forced_modes):
        local = density.shape
        size_x, size_y, size_z = local
        rows = size_x * size_y
        full = (size_x * sizes["gx"], size_y * sizes["gy"], size_z * sizes["gz"])
        early, late = tables(local, full)
        modes = forced_modes.T
        stages = plan(sizes)
        messages = sum(len(g) for g in stages)
        any_spec = pl.BlockSpec(memory_space=pl.ANY)
        f32 = jnp.float32
        return tuple(pl.pallas_call(
            functools.partial(kernel, sizes, local),
            out_shape=[jax.ShapeDtypeStruct(local, f32)] * 3,
            in_specs=[any_spec] * 6,
            out_specs=[any_spec] * 3,
            scratch_shapes=[
                pltpu.VMEM((3, size_x + 2 * REACH, size_y, size_z), f32),
                pltpu.VMEM(modes.shape, jnp.int32),
                pltpu.VMEM(early.shape, f32),
                pltpu.VMEM(late.shape, f32),
                pltpu.VMEM((2, size_x, size_y + 16, size_z), f32),
                pltpu.VMEM((2, 2, size_x, 8, size_z), f32),
                pltpu.VMEM((2, size_x, 8, size_z), f32),
                pltpu.VMEM((2, 8, rows), f32),
                pltpu.VMEM((2, 2, 8, rows), f32),
                pltpu.VMEM((len(stages), 8, 2 * HALF), f32),
                pltpu.VMEM((messages, 8, 2 * HALF), f32),
                pltpu.VMEM((3,) + tuple(local), f32),
                pltpu.SemaphoreType.DMA((6,)),
                pltpu.SemaphoreType.DMA((3,)),
                pltpu.SemaphoreType.DMA((6,)),
                pltpu.SemaphoreType.DMA((6,)),
                pltpu.SemaphoreType.DMA((messages,)),
                pltpu.SemaphoreType.DMA((messages,)),
            ],
            compiler_params=pltpu.CompilerParams(collective_id=0, has_side_effects=True),
            name="flame",
        )(density, momentum, hydrogen, modes, jnp.asarray(early), jnp.asarray(late)))

    in_specs = (P("gx", "gy", "gz"), P("gx", "gy", "gz"), P("gx", "gy", "gz"), P())
    out_specs = (P("gx", "gy", "gz"), P("gx", "gy", "gz"), P("gx", "gy", "gz"))
    return jax.shard_map(
        per_device, mesh=mesh, in_specs=in_specs, out_specs=out_specs, check_vma=False
    )
```

```python
import functools
import math

import jax
import jax.numpy as jnp
import numpy as np
from jax import lax
from jax.experimental import pallas as pl
from jax.experimental.pallas import tpu as pltpu
from jax.sharding import PartitionSpec as P

KMAX = 3
WIDTH = 2 * KMAX + 1
HALF = 64
REACH = 4

FIRST_COEFFS = (0.8, -0.2, 4.0 / 105.0, -1.0 / 280.0)
SECOND_COEFFS = (1.6, -0.2, 8.0 / 315.0, -1.0 / 560.0)
CENTRE_COEFF = -205.0 / 72.0
VISCOSITY = 0.3
DIFFUSIVITY = 1.5
FORCE_POWER = 0.3
ENERGY_EPS = 1e-06
ACTIVATION = 2.0
HIGHEST = lax.Precision.HIGHEST
MESH = pl.DeviceIdType.MESH


def tables(local, full):
    size_x, size_y, size_z = local
    full_x, full_y, full_z = full
    k = np.arange(-KMAX, KMAX + 1)
    ang_z = 2.0 * np.pi * (k[:, None] * np.arange(size_z)[None, :]) / full_z
    trig_z = np.zeros((16, size_z))
    trig_z[:WIDTH] = np.cos(ang_z)
    trig_z[8 : 8 + WIDTH] = np.sin(ang_z)
    ax = k[:, None] * np.arange(size_x)[None, :] / full_x
    ay = k[:, None] * np.arange(size_y)[None, :] / full_y
    ang = 2.0 * np.pi * (ax[:, None, :, None] + ay[None, :, None, :])
    ang = ang.reshape(WIDTH * WIDTH, size_x * size_y)
    trig_xy = np.zeros((2 * HALF, size_x * size_y))
    trig_xy[: WIDTH * WIDTH] = np.cos(ang)
    trig_xy[HALF : HALF + WIDTH * WIDTH] = np.sin(ang)
    edge = np.zeros((8, size_z))
    for j in range(REACH):
        edge[j, j] = 1.0
        edge[REACH + j, size_z - REACH + j] = 1.0
    band = np.zeros((size_z, size_z))
    halo = np.zeros((16, size_z))
    for z in range(size_z):
        band[z, z] = 3.0 * CENTRE_COEFF
        for offset, weight in enumerate(SECOND_COEFFS, 1):
            for q in (z - offset, z + offset):
                if 0 <= q < size_z:
                    band[q, z] = weight
                elif q < 0:
                    halo[8 + q, z] = weight
                else:
                    halo[8 + q - size_z, z] = weight
    early = np.concatenate([trig_z, edge, trig_xy], 0).astype(np.float32)
    late = np.concatenate([halo, band], 0).astype(np.float32)
    return early, late


def dot_nt(a, b):
    return lax.dot_general(a, b, (((1,), (1,)), ((), ())), precision=HIGHEST, preferred_element_type=jnp.float32)


def dot_nn(a, b):
    return lax.dot_general(a, b, (((1,), (0,)), ((), ())), precision=HIGHEST, preferred_element_type=jnp.float32)


def dot_tn(a, b):
    return lax.dot_general(a, b, (((0,), (0,)), ((), ())), precision=HIGHEST, preferred_element_type=jnp.float32)


def group_offsets(sizes, axes):
    offsets = [{}]
    for axis in axes:
        offsets = [{**o, axis: s} for o in offsets for s in range(sizes[axis])]
    return [o for o in offsets if any(o.values())]


def tree_sum(parts):
    parts = list(parts)
    while len(parts) > 1:
        parts = [sum(parts[i : i + 2][1:], parts[i]) for i in range(0, len(parts), 2)]
    return parts[0]


def plan(sizes):
    if sizes["gx"] * sizes["gy"] <= 16:
        stages = [("gz",), ("gx", "gy")]
    else:
        stages = [("gz",), ("gx",), ("gy",)]
    return [group_offsets(sizes, s) for s in stages]


def kernel(sizes, local, dens_hbm, mom_hbm, fuel_hbm, modes_hbm, early_hbm, late_hbm,
           drate, mrate, hrate,
           f, modes, early, late, edges, sides, ypack, zpack, ztile, stage_own, stage_got,
           load_sem, halo_send, halo_recv, stage_send, stage_recv):
    size_x, size_y, size_z = local
    rows = size_x * size_y
    me = {a: lax.axis_index(a) for a in sizes}
    stages = plan(sizes)

    def at(offset):
        return {a: lax.rem(me[a] + o, sizes[a]) for a, o in offset.items()}

    own = pl.ds(REACH, size_x)
    loads = [
        pltpu.make_async_copy(src, dst, load_sem.at[i])
        for i, (src, dst) in enumerate([
            (dens_hbm, f.at[0, own]), (mom_hbm, f.at[1, own]), (early_hbm, early),
            (fuel_hbm, f.at[2, own]), (modes_hbm, modes), (late_hbm, late),
        ])
    ]
    for copy in loads:
        copy.start()
    barrier = pltpu.get_barrier_semaphore()
    partners = [o for group in stages for o in group]
    for offset in partners:
        pl.semaphore_signal(barrier, inc=1, device_id=at(offset), device_id_type=MESH)

    row = lax.broadcasted_iota(jnp.int32, (8, 2 * HALF), 0)
    lane = lax.broadcasted_iota(jnp.int32, (8, 2 * HALF), 1)
    pair = lax.rem(lane, HALF)
    kx = lax.div(pair, WIDTH)
    ky = pair - kx * WIDTH
    turn = jnp.zeros((8, 2 * HALF), jnp.float32)
    for k, axis, size in ((kx, "gx", size_x), (ky, "gy", size_y), (row, "gz", size_z)):
        count = (k - KMAX).astype(jnp.float32) * me[axis].astype(jnp.float32)
        part = count / sizes[axis]
        turn = turn + (part - jnp.floor(part))
    turn = turn - jnp.floor(turn + 0.5)
    cos_p = jnp.cos(2.0 * math.pi * turn)
    sin_p = jnp.sin(2.0 * math.pi * turn)
    sign = jnp.where(lane < HALF, -1.0, 1.0)
    sin_p = sign * sin_p

    loads[0].wait()
    loads[1].wait()
    loads[2].wait()
    flat = lambda i: f[i, own].reshape(rows, size_z)
    vel = flat(1) / flat(0)
    trig_z = early[0:16]
    trig_xy = early[24 : 24 + 2 * HALF]
    grid = dot_nt(dot_nt(trig_z, vel), trig_xy)
    cube = grid[0:8] + sign * pltpu.roll(grid[8:16], HALF, 1)
    cube = cos_p * cube + sin_p * pltpu.roll(cube, HALF, 1)
    stage_own[0] = cube

    def send_stage(s):
        base = sum(len(g) for g in stages[:s])
        copies = []
        for i, offset in enumerate(stages[s]):
            copy = pltpu.make_async_remote_copy(
                src_ref=stage_own.at[s], dst_ref=stage_got.at[base + i],
                send_sem=stage_send.at[base + i], recv_sem=stage_recv.at[base + i],
                device_id=at(offset), device_id_type=MESH)
            copy.start()
            copies.append(copy)
        return copies

    def sum_stage(s, copies):
        base = sum(len(g) for g in stages[:s])
        for copy in copies:
            copy.wait_recv()
        return tree_sum([stage_own[s]] + [stage_got[base + i] for i in range(len(copies))])

    pl.semaphore_wait(barrier, len(partners))
    pending = send_stage(0)
    started = list(pending)
    loads[3].wait()

    def send(src, dst, slot, axis, step):
        copy = pltpu.make_async_remote_copy(
            src_ref=src, dst_ref=dst, send_sem=halo_send.at[slot], recv_sem=halo_recv.at[slot],
            device_id=at({axis: step % sizes[axis]}), device_id_type=MESH)
        copy.start()
        return copy

    halos_x = [
        send(f.at[:, pl.ds(size_x, REACH)], f.at[:, pl.ds(0, REACH)], 0, "gx", 1),
        send(f.at[:, pl.ds(REACH, REACH)], f.at[:, pl.ds(size_x + REACH, REACH)], 1, "gx", -1),
    ]
    for i in range(2):
        ypack[i, :, 0:REACH] = f[1 + i, own, 0:REACH]
        ypack[i, :, REACH : 2 * REACH] = f[1 + i, own, size_y - REACH : size_y]
        zpack[i] = dot_nt(early[16:24], flat(1 + i))
    halos_y = [send(ypack, sides.at[0], 2, "gy", 1)]
    if sizes["gy"] > 2:
        halos_y.append(send(ypack, sides.at[1], 3, "gy", -1))
    halos_z = [send(zpack, ztile.at[0], 4, "gz", 1), send(zpack, ztile.at[1], 5, "gz", -1)]

    loads[4].wait()
    hit_z = lax.broadcasted_iota(jnp.int32, (8, modes.shape[1]), 0) == modes[2:3] + KMAX
    code = (modes[0:1] + KMAX) * WIDTH + modes[1:2] + KMAX
    hit_xy = lax.rem(lax.broadcasted_iota(jnp.int32, (2 * HALF, modes.shape[1]), 0), HALF) == code
    chosen = dot_nt(hit_z.astype(jnp.float32), hit_xy.astype(jnp.float32))

    loads[5].wait()
    lap = [dot_nn(flat(1 + i), late[16 : 16 + size_z]).reshape(size_x, size_y, size_z) for i in range(2)]
    outs = (drate, mrate, hrate)
    mrate[...] = lap[0]
    hrate[...] = lap[1]

    for s in range(1, len(stages)):
        stage_own[s] = sum_stage(s - 1, pending)
        pending = send_stage(s)
        started += pending

    for copy in halos_z:
        copy.wait_recv()
    for copy in halos_y:
        copy.wait_recv()
    for i in range(2):
        tile = jnp.concatenate([ztile[0, i], ztile[1, i]], 0)
        edges[i, :, 0:8] = sides[0, i]
        edges[i, :, 8 : 8 + size_y] = f[1 + i, own]
        edges[i, :, 8 + size_y : 16 + size_y] = sides[1 if sizes["gy"] > 2 else 0, i]
        total = outs[1 + i][...] + dot_tn(tile, late[0:16]).reshape(size_x, size_y, size_z)
        for offset, weight in enumerate(SECOND_COEFFS, 1):
            total = total + weight * (
                edges[i, :, 8 + offset : 8 + offset + size_y] + edges[i, :, 8 - offset : 8 - offset + size_y])
        outs[1 + i][...] = total

    for copy in halos_x:
        copy.wait_recv()
    def planes(x, offset):
        return x[REACH + offset : REACH + offset + size_x]

    def first_diff(x):
        total = None
        for offset, weight in enumerate(FIRST_COEFFS, 1):
            term = weight * (planes(x, offset) - planes(x, -offset))
            total = term if total is None else total + term
        return total

    def second_diff(x):
        return tree_sum([w * (planes(x, o) + planes(x, -o)) for o, w in enumerate(SECOND_COEFFS, 1)])

    mom = f[1]
    dens = f[0]
    fuel = f[2]
    vel_pad = mom / dens
    drate[...] = -first_diff(mom)
    mid_fuel = planes(fuel, 0)
    hrate[...] = (DIFFUSIVITY * (hrate[...] + second_diff(fuel)) - first_diff(fuel * vel_pad)
                  - mid_fuel * jnp.exp(-ACTIVATION * mid_fuel / planes(dens, 0)))
    mrate[...] = VISCOSITY * (mrate[...] + second_diff(mom)) - first_diff(mom * vel_pad + dens)

    ncell = float(rows * size_z * math.prod(sizes.values()))
    cube = sum_stage(len(stages) - 1, pending)
    coef = chosen * cube / ncell
    energy = jnp.sum(jnp.sum(coef * coef, axis=1, keepdims=True), axis=0, keepdims=True)
    scale = 2.0 * FORCE_POWER / (energy + ENERGY_EPS)
    local_coef = cos_p * coef - sin_p * pltpu.roll(coef, HALF, 1)
    both = jnp.concatenate([local_coef, -sign * pltpu.roll(local_coef, HALF, 1)], 0)
    low = dot_tn(dot_nn(both, trig_xy), trig_z).reshape(size_x, size_y, size_z)
    mrate[...] = mrate[...] + f[0, own] * (low * scale.reshape(1, 1, 1))
    for copy in started + halos_x + halos_y + halos_z:
        copy.wait_send()


def write_out(*refs):
    count = len(refs) // 2
    copies = [pltpu.make_async_copy(refs[i], refs[count + i], refs[-1].at[i]) for i in range(count)]
    for copy in copies:
        copy.start()
    for copy in copies:
        copy.wait()


def solution(mesh):
    sizes = {a: mesh.shape[a] for a in ("gx", "gy", "gz")}

    def per_device(density, momentum, hydrogen, forced_modes):
        local = density.shape
        size_x, size_y, size_z = local
        rows = size_x * size_y
        full = (size_x * sizes["gx"], size_y * sizes["gy"], size_z * sizes["gz"])
        early, late = tables(local, full)
        modes = forced_modes.T
        stages = plan(sizes)
        messages = sum(len(g) for g in stages)
        any_spec = pl.BlockSpec(memory_space=pl.ANY)
        f32 = jnp.float32
        rates = pl.pallas_call(
            functools.partial(kernel, sizes, local),
            out_shape=[pltpu.VMEM(local, f32)] * 3,
            in_specs=[any_spec] * 6,
            out_specs=[pl.BlockSpec(memory_space=pltpu.VMEM)] * 3,
            scratch_shapes=[
                pltpu.VMEM((3, size_x + 2 * REACH, size_y, size_z), f32),
                pltpu.VMEM(modes.shape, jnp.int32),
                pltpu.VMEM(early.shape, f32),
                pltpu.VMEM(late.shape, f32),
                pltpu.VMEM((2, size_x, size_y + 16, size_z), f32),
                pltpu.VMEM((2, 2, size_x, 8, size_z), f32),
                pltpu.VMEM((2, size_x, 8, size_z), f32),
                pltpu.VMEM((2, 8, rows), f32),
                pltpu.VMEM((2, 2, 8, rows), f32),
                pltpu.VMEM((len(stages), 8, 2 * HALF), f32),
                pltpu.VMEM((messages, 8, 2 * HALF), f32),
                pltpu.SemaphoreType.DMA((6,)),
                pltpu.SemaphoreType.DMA((6,)),
                pltpu.SemaphoreType.DMA((6,)),
                pltpu.SemaphoreType.DMA((messages,)),
                pltpu.SemaphoreType.DMA((messages,)),
            ],
            compiler_params=pltpu.CompilerParams(collective_id=0, has_side_effects=True),
            name="flame",
        )(density, momentum, hydrogen, modes, jnp.asarray(early), jnp.asarray(late))
        return tuple(pl.pallas_call(
            write_out,
            out_shape=[jax.ShapeDtypeStruct(local, f32)] * 3,
            in_specs=[pl.BlockSpec(memory_space=pltpu.VMEM)] * 3,
            out_specs=[any_spec] * 3,
            scratch_shapes=[pltpu.SemaphoreType.DMA((3,))],
            name="write",
        )(*[pltpu.with_memory_space_constraint(r, pltpu.VMEM) for r in rates]))

    in_specs = (P("gx", "gy", "gz"), P("gx", "gy", "gz"), P("gx", "gy", "gz"), P())
    out_specs = (P("gx", "gy", "gz"), P("gx", "gy", "gz"), P("gx", "gy", "gz"))
    return jax.shard_map(
        per_device, mesh=mesh, in_specs=in_specs, out_specs=out_specs, check_vma=False
    )
```

```python
import functools
import math

import jax
import jax.numpy as jnp
import numpy as np
from jax import lax
from jax.experimental import pallas as pl
from jax.experimental.pallas import tpu as pltpu
from jax.sharding import PartitionSpec as P

KMAX = 3
WIDTH = 2 * KMAX + 1
HALF = 64
ROWS = KMAX + 1
REACH = 4

FIRST_COEFFS = (0.8, -0.2, 4.0 / 105.0, -1.0 / 280.0)
SECOND_COEFFS = (1.6, -0.2, 8.0 / 315.0, -1.0 / 560.0)
CENTRE_COEFF = -205.0 / 72.0
VISCOSITY = 0.3
DIFFUSIVITY = 1.5
FORCE_POWER = 0.3
ENERGY_EPS = 1e-06
ACTIVATION = 2.0
HIGHEST = lax.Precision.HIGHEST
MESH = pl.DeviceIdType.MESH


def tables(local, full):
    size_x, size_y, size_z = local
    full_x, full_y, full_z = full
    k = np.arange(-KMAX, KMAX + 1)
    ang_z = 2.0 * np.pi * (k[:, None] * np.arange(size_z)[None, :]) / full_z
    trig_z = np.zeros((2 * ROWS, size_z))
    trig_z[:ROWS] = np.cos(ang_z[KMAX:])
    trig_z[ROWS:] = np.sin(ang_z[KMAX:])
    ax = k[:, None] * np.arange(size_x)[None, :] / full_x
    ay = k[:, None] * np.arange(size_y)[None, :] / full_y
    ang = 2.0 * np.pi * (ax[:, None, :, None] + ay[None, :, None, :])
    ang = ang.reshape(WIDTH * WIDTH, size_x * size_y)
    trig_xy = np.zeros((2 * HALF, size_x * size_y))
    trig_xy[: WIDTH * WIDTH] = np.cos(ang)
    trig_xy[HALF : HALF + WIDTH * WIDTH] = np.sin(ang)
    edge = np.zeros((8, size_z))
    for j in range(REACH):
        edge[j, j] = 1.0
        edge[REACH + j, size_z - REACH + j] = 1.0
    band = np.zeros((size_z, size_z))
    halo = np.zeros((16, size_z))
    for z in range(size_z):
        band[z, z] = 3.0 * CENTRE_COEFF
        for offset, weight in enumerate(SECOND_COEFFS, 1):
            for q in (z - offset, z + offset):
                if 0 <= q < size_z:
                    band[q, z] = weight
                elif q < 0:
                    halo[8 + q, z] = weight
                else:
                    halo[8 + q - size_z, z] = weight
    z_high, z_low = split_host(trig_z)
    xy_high, xy_low = split_host(trig_xy)
    early = np.concatenate([z_high, z_low, xy_high, xy_low, z_high, z_high, z_low, z_low], 0)
    back = np.concatenate([xy_high, xy_low], 1)
    late = np.concatenate([edge, halo, band], 0).astype(np.float32)
    return early, back, late


def split_host(table):
    high = table.astype(np.float32).astype(jnp.bfloat16)
    low = (table - high.astype(np.float64)).astype(np.float32).astype(jnp.bfloat16)
    return high, low


def split(x):
    high = x.astype(jnp.bfloat16).astype(jnp.float32)
    return high, x - high


def dot_split(a, b, contract):
    return lax.dot_general(a.astype(jnp.bfloat16), b.astype(jnp.bfloat16), (contract, ((), ())),
                           preferred_element_type=jnp.float32)


def fold(x):
    rows, lanes = x.shape
    x = x[: rows // 2] + x[rows // 2 :]
    return x[:, : lanes // 2] + x[:, lanes // 2 :]


def dot_nt(a, b):
    return lax.dot_general(a, b, (((1,), (1,)), ((), ())), precision=HIGHEST, preferred_element_type=jnp.float32)


def dot_nn(a, b):
    return lax.dot_general(a, b, (((1,), (0,)), ((), ())), precision=HIGHEST, preferred_element_type=jnp.float32)


def dot_tn(a, b):
    return lax.dot_general(a, b, (((0,), (0,)), ((), ())), precision=HIGHEST, preferred_element_type=jnp.float32)


def group_offsets(sizes, axes):
    offsets = [{}]
    for axis in axes:
        offsets = [{**o, axis: s} for o in offsets for s in range(sizes[axis])]
    return [o for o in offsets if any(o.values())]


def tree_sum(parts):
    parts = list(parts)
    while len(parts) > 1:
        parts = [sum(parts[i : i + 2][1:], parts[i]) for i in range(0, len(parts), 2)]
    return parts[0]


def plan(sizes):
    if sizes["gx"] * sizes["gy"] <= 16:
        stages = [("gz",), ("gx", "gy")]
    else:
        stages = [("gz",), ("gx",), ("gy",)]
    return [group_offsets(sizes, s) for s in stages]


def kernel(sizes, local, dens_hbm, mom_hbm, fuel_hbm, modes_hbm, early_hbm, back_hbm, late_hbm,
           drate, mrate, hrate,
           f, modes, early, back, late, edges, sides, ypack, zpack, ztile, stage_own, stage_got,
           load_sem, halo_send, halo_recv, stage_send, stage_recv):
    size_x, size_y, size_z = local
    rows = size_x * size_y
    rows_z = 2 * ROWS
    me = {a: lax.axis_index(a) for a in sizes}
    stages = plan(sizes)

    def at(offset):
        return {a: lax.rem(me[a] + o, sizes[a]) for a, o in offset.items()}

    own = pl.ds(REACH, size_x)
    loads = [
        pltpu.make_async_copy(src, dst, load_sem.at[i])
        for i, (src, dst) in enumerate([
            (dens_hbm, f.at[0, own]), (mom_hbm, f.at[1, own]), (early_hbm, early),
            (fuel_hbm, f.at[2, own]), (modes_hbm, modes), (late_hbm, late), (back_hbm, back),
        ])
    ]
    for copy in loads:
        copy.start()
    barrier = pltpu.get_barrier_semaphore()
    partners = [o for group in stages for o in group]
    for offset in partners:
        pl.semaphore_signal(barrier, inc=1, device_id=at(offset), device_id_type=MESH)

    row = lax.broadcasted_iota(jnp.int32, (ROWS, 2 * HALF), 0)
    lane = lax.broadcasted_iota(jnp.int32, (ROWS, 2 * HALF), 1)
    pair = lax.rem(lane, HALF)
    kx = lax.div(pair, WIDTH)
    ky = pair - kx * WIDTH
    turn = jnp.zeros((ROWS, 2 * HALF), jnp.float32)
    for k, axis, size in ((kx - KMAX, "gx", size_x), (ky - KMAX, "gy", size_y), (row, "gz", size_z)):
        count = k.astype(jnp.float32) * me[axis].astype(jnp.float32)
        part = count / sizes[axis]
        turn = turn + (part - jnp.floor(part))
    turn = turn - jnp.floor(turn + 0.5)
    cos_p = jnp.cos(2.0 * math.pi * turn)
    sin_p = jnp.sin(2.0 * math.pi * turn)
    sign = jnp.where(lane < HALF, -1.0, 1.0)
    sin_p = sign * sin_p

    loads[0].wait()
    loads[1].wait()
    loads[2].wait()
    flat = lambda i: f[i, own].reshape(rows, size_z)
    vel = flat(1) / flat(0)
    deep = 2 * rows_z
    table_xy = early[deep : deep + 4 * HALF]
    vel_both = jnp.concatenate(split(vel), 0)
    part = fold(dot_split(early[0:deep], vel_both, ((1,), (1,))))
    grid = fold(dot_split(jnp.concatenate(split(part), 0), table_xy, ((1,), (1,))))
    cube = grid[0:ROWS] + sign * pltpu.roll(grid[ROWS:], HALF, 1)
    cube = cos_p * cube + sin_p * pltpu.roll(cube, HALF, 1)
    stage_own[0] = cube

    def send_stage(s):
        base = sum(len(g) for g in stages[:s])
        copies = []
        for i, offset in enumerate(stages[s]):
            copy = pltpu.make_async_remote_copy(
                src_ref=stage_own.at[s], dst_ref=stage_got.at[base + i],
                send_sem=stage_send.at[base + i], recv_sem=stage_recv.at[base + i],
                device_id=at(offset), device_id_type=MESH)
            copy.start()
            copies.append(copy)
        return copies

    def sum_stage(s, copies):
        base = sum(len(g) for g in stages[:s])
        for copy in copies:
            copy.wait_recv()
        return tree_sum([stage_own[s]] + [stage_got[base + i] for i in range(len(copies))])

    pl.semaphore_wait(barrier, len(partners))
    pending = send_stage(0)
    started = list(pending)
    loads[3].wait()

    def send(src, dst, slot, axis, step):
        copy = pltpu.make_async_remote_copy(
            src_ref=src, dst_ref=dst, send_sem=halo_send.at[slot], recv_sem=halo_recv.at[slot],
            device_id=at({axis: step % sizes[axis]}), device_id_type=MESH)
        copy.start()
        return copy

    loads[5].wait()
    halos_x = [
        send(f.at[:, pl.ds(size_x, REACH)], f.at[:, pl.ds(0, REACH)], 0, "gx", 1),
        send(f.at[:, pl.ds(REACH, REACH)], f.at[:, pl.ds(size_x + REACH, REACH)], 1, "gx", -1),
    ]
    for i in range(2):
        ypack[i, :, 0:REACH] = f[1 + i, own, 0:REACH]
        ypack[i, :, REACH : 2 * REACH] = f[1 + i, own, size_y - REACH : size_y]
        zpack[i] = dot_nt(late[0:8], flat(1 + i))
    halos_y = [send(ypack, sides.at[0], 2, "gy", 1)]
    if sizes["gy"] > 2:
        halos_y.append(send(ypack, sides.at[1], 3, "gy", -1))
    halos_z = [send(zpack, ztile.at[0], 4, "gz", 1), send(zpack, ztile.at[1], 5, "gz", -1)]

    loads[4].wait()
    count = modes.shape[1]
    row_z = lax.broadcasted_iota(jnp.int32, (ROWS, count), 0)
    row_xy = lax.rem(lax.broadcasted_iota(jnp.int32, (2 * HALF, count), 0), HALF)
    code = (modes[0:1] + KMAX) * WIDTH + modes[1:2] + KMAX
    hits = [((row_z == modes[2:3]), (row_xy == code)),
            ((row_z == -modes[2:3]) & (row_z > 0), (row_xy == WIDTH * WIDTH - 1 - code))]
    chosen = sum(dot_nt(hz.astype(jnp.float32), hxy.astype(jnp.float32)) for hz, hxy in hits)

    lap = [dot_nn(flat(1 + i), late[24 : 24 + size_z]).reshape(size_x, size_y, size_z) for i in range(2)]
    outs = (drate, mrate, hrate)
    mrate[...] = lap[0]
    hrate[...] = lap[1]

    for s in range(1, len(stages)):
        stage_own[s] = sum_stage(s - 1, pending)
        pending = send_stage(s)
        started += pending

    for copy in halos_z:
        copy.wait_recv()
    for copy in halos_y:
        copy.wait_recv()
    for i in range(2):
        tile = jnp.concatenate([ztile[0, i], ztile[1, i]], 0)
        edges[i, :, 0:8] = sides[0, i]
        edges[i, :, 8 : 8 + size_y] = f[1 + i, own]
        edges[i, :, 8 + size_y : 16 + size_y] = sides[1 if sizes["gy"] > 2 else 0, i]
        total = outs[1 + i][...] + dot_tn(tile, late[8:24]).reshape(size_x, size_y, size_z)
        for offset, weight in enumerate(SECOND_COEFFS, 1):
            total = total + weight * (
                edges[i, :, 8 + offset : 8 + offset + size_y] + edges[i, :, 8 - offset : 8 - offset + size_y])
        outs[1 + i][...] = total

    for copy in halos_x:
        copy.wait_recv()
    def planes(x, offset):
        return x[REACH + offset : REACH + offset + size_x]

    def first_diff(x):
        total = None
        for offset, weight in enumerate(FIRST_COEFFS, 1):
            term = weight * (planes(x, offset) - planes(x, -offset))
            total = term if total is None else total + term
        return total

    def second_diff(x):
        return tree_sum([w * (planes(x, o) + planes(x, -o)) for o, w in enumerate(SECOND_COEFFS, 1)])

    mom = f[1]
    dens = f[0]
    fuel = f[2]
    vel_pad = mom / dens
    drate[...] = -first_diff(mom)
    mid_fuel = planes(fuel, 0)
    hrate[...] = (DIFFUSIVITY * (hrate[...] + second_diff(fuel)) - first_diff(fuel * vel_pad)
                  - mid_fuel * jnp.exp(-ACTIVATION * mid_fuel / planes(dens, 0)))
    mrate[...] = VISCOSITY * (mrate[...] + second_diff(mom)) - first_diff(mom * vel_pad + dens)

    loads[6].wait()
    ncell = float(rows * size_z * math.prod(sizes.values()))
    cube = sum_stage(len(stages) - 1, pending)
    coef = cube / ncell
    picked = chosen * coef
    energy = jnp.sum(jnp.sum(picked * coef, axis=1, keepdims=True), axis=0, keepdims=True)
    scale = 2.0 * FORCE_POWER / (energy + ENERGY_EPS)
    local_coef = cos_p * picked - sin_p * pltpu.roll(picked, HALF, 1)
    both = jnp.concatenate([local_coef, -sign * pltpu.roll(local_coef, HALF, 1)], 0)
    wave = fold(dot_split(jnp.concatenate(split(both), 0), back[...], ((1,), (0,))))
    high, rest = split(wave)
    waves = jnp.concatenate([high, rest, high, rest], 0).T
    low = dot_split(waves, early[deep + 4 * HALF : deep + 4 * HALF + 4 * rows_z], ((1,), (0,)))
    low = low.reshape(size_x, size_y, size_z)
    mrate[...] = mrate[...] + f[0, own] * (low * scale.reshape(1, 1, 1))
    for copy in started + halos_x + halos_y + halos_z:
        copy.wait_send()


def write_out(*refs):
    count = len(refs) // 2
    copies = [pltpu.make_async_copy(refs[i], refs[count + i], refs[-1].at[i]) for i in range(count)]
    for copy in copies:
        copy.start()
    for copy in copies:
        copy.wait()


def solution(mesh):
    sizes = {a: mesh.shape[a] for a in ("gx", "gy", "gz")}

    def per_device(density, momentum, hydrogen, forced_modes):
        local = density.shape
        size_x, size_y, size_z = local
        rows = size_x * size_y
        full = (size_x * sizes["gx"], size_y * sizes["gy"], size_z * sizes["gz"])
        early, back, late = tables(local, full)
        modes = forced_modes.T
        stages = plan(sizes)
        messages = sum(len(g) for g in stages)
        any_spec = pl.BlockSpec(memory_space=pl.ANY)
        f32 = jnp.float32
        rates = pl.pallas_call(
            functools.partial(kernel, sizes, local),
            out_shape=[pltpu.VMEM(local, f32)] * 3,
            in_specs=[any_spec] * 7,
            out_specs=[pl.BlockSpec(memory_space=pltpu.VMEM)] * 3,
            scratch_shapes=[
                pltpu.VMEM((3, size_x + 2 * REACH, size_y, size_z), f32),
                pltpu.VMEM(modes.shape, jnp.int32),
                pltpu.VMEM(early.shape, jnp.bfloat16),
                pltpu.VMEM(back.shape, jnp.bfloat16),
                pltpu.VMEM(late.shape, f32),
                pltpu.VMEM((2, size_x, size_y + 16, size_z), f32),
                pltpu.VMEM((2, 2, size_x, 8, size_z), f32),
                pltpu.VMEM((2, size_x, 8, size_z), f32),
                pltpu.VMEM((2, 8, rows), f32),
                pltpu.VMEM((2, 2, 8, rows), f32),
                pltpu.VMEM((len(stages), ROWS, 2 * HALF), f32),
                pltpu.VMEM((messages, ROWS, 2 * HALF), f32),
                pltpu.SemaphoreType.DMA((7,)),
                pltpu.SemaphoreType.DMA((6,)),
                pltpu.SemaphoreType.DMA((6,)),
                pltpu.SemaphoreType.DMA((messages,)),
                pltpu.SemaphoreType.DMA((messages,)),
            ],
            compiler_params=pltpu.CompilerParams(collective_id=0, has_side_effects=True),
            name="flame",
        )(density, momentum, hydrogen, modes, jnp.asarray(early), jnp.asarray(back), jnp.asarray(late))
        return tuple(pl.pallas_call(
            write_out,
            out_shape=[jax.ShapeDtypeStruct(local, f32)] * 3,
            in_specs=[pl.BlockSpec(memory_space=pltpu.VMEM)] * 3,
            out_specs=[any_spec] * 3,
            scratch_shapes=[pltpu.SemaphoreType.DMA((3,))],
            name="write",
        )(*[pltpu.with_memory_space_constraint(r, pltpu.VMEM) for r in rates]))

    in_specs = (P("gx", "gy", "gz"), P("gx", "gy", "gz"), P("gx", "gy", "gz"), P())
    out_specs = (P("gx", "gy", "gz"), P("gx", "gy", "gz"), P("gx", "gy", "gz"))
    return jax.shard_map(
        per_device, mesh=mesh, in_specs=in_specs, out_specs=out_specs, check_vma=False
    )
```

```python
import functools
import math

import jax
import jax.numpy as jnp
import numpy as np
from jax import lax
from jax.experimental import pallas as pl
from jax.experimental.pallas import tpu as pltpu
from jax.sharding import PartitionSpec as P

KMAX = 3
WIDTH = 2 * KMAX + 1
HALF = 64
ROWS = KMAX + 1
REACH = 4

FIRST_COEFFS = (0.8, -0.2, 4.0 / 105.0, -1.0 / 280.0)
SECOND_COEFFS = (1.6, -0.2, 8.0 / 315.0, -1.0 / 560.0)
CENTRE_COEFF = -205.0 / 72.0
VISCOSITY = 0.3
DIFFUSIVITY = 1.5
FORCE_POWER = 0.3
ENERGY_EPS = 1e-06
ACTIVATION = 2.0
HIGHEST = lax.Precision.HIGHEST
MESH = pl.DeviceIdType.MESH


def tables(local, full):
    size_x, size_y, size_z = local
    full_x, full_y, full_z = full
    k = np.arange(-KMAX, KMAX + 1)
    ang_z = 2.0 * np.pi * (k[:, None] * np.arange(size_z)[None, :]) / full_z
    trig_z = np.zeros((2 * ROWS, size_z))
    trig_z[:ROWS] = np.cos(ang_z[KMAX:])
    trig_z[ROWS:] = np.sin(ang_z[KMAX:])
    ax = k[:, None] * np.arange(size_x)[None, :] / full_x
    ay = k[:, None] * np.arange(size_y)[None, :] / full_y
    ang = 2.0 * np.pi * (ax[:, None, :, None] + ay[None, :, None, :])
    ang = ang.reshape(WIDTH * WIDTH, size_x * size_y)
    trig_xy = np.zeros((2 * HALF, size_x * size_y))
    trig_xy[: WIDTH * WIDTH] = np.cos(ang)
    trig_xy[HALF : HALF + WIDTH * WIDTH] = np.sin(ang)
    edge = np.zeros((8, size_z))
    for j in range(REACH):
        edge[j, j] = 1.0
        edge[REACH + j, size_z - REACH + j] = 1.0
    band = np.zeros((size_z, size_z))
    halo = np.zeros((16, size_z))
    for z in range(size_z):
        band[z, z] = 3.0 * CENTRE_COEFF
        for offset, weight in enumerate(SECOND_COEFFS, 1):
            for q in (z - offset, z + offset):
                if 0 <= q < size_z:
                    band[q, z] = weight
                elif q < 0:
                    halo[8 + q, z] = weight
                else:
                    halo[8 + q - size_z, z] = weight
    z_high, z_low = split_host(trig_z)
    xy_high, xy_low = split_host(trig_xy)
    early = np.concatenate([z_high, z_low, xy_high, xy_low, z_high, z_high, z_low, z_low], 0)
    back = np.concatenate([xy_high, xy_low], 1)
    late = np.concatenate([edge, halo, band], 0).astype(np.float32)
    return early, back, late


def split_host(table):
    high = table.astype(np.float32).astype(jnp.bfloat16)
    low = (table - high.astype(np.float64)).astype(np.float32).astype(jnp.bfloat16)
    return high, low


def split(x):
    high = x.astype(jnp.bfloat16).astype(jnp.float32)
    return high, x - high


def dot_split(a, b, contract):
    return lax.dot_general(a.astype(jnp.bfloat16), b.astype(jnp.bfloat16), (contract, ((), ())),
                           preferred_element_type=jnp.float32)


def fold(x):
    rows, lanes = x.shape
    x = x[: rows // 2] + x[rows // 2 :]
    return x[:, : lanes // 2] + x[:, lanes // 2 :]


def dot_nt(a, b):
    return lax.dot_general(a, b, (((1,), (1,)), ((), ())), precision=HIGHEST, preferred_element_type=jnp.float32)


def dot_nn(a, b):
    return lax.dot_general(a, b, (((1,), (0,)), ((), ())), precision=HIGHEST, preferred_element_type=jnp.float32)


def dot_tn(a, b):
    return lax.dot_general(a, b, (((0,), (0,)), ((), ())), precision=HIGHEST, preferred_element_type=jnp.float32)


def group_offsets(sizes, axes):
    offsets = [{}]
    for axis in axes:
        offsets = [{**o, axis: s} for o in offsets for s in range(sizes[axis])]
    return [o for o in offsets if any(o.values())]


def tree_sum(parts):
    parts = list(parts)
    while len(parts) > 1:
        parts = [sum(parts[i : i + 2][1:], parts[i]) for i in range(0, len(parts), 2)]
    return parts[0]


def plan(sizes):
    if math.prod(sizes.values()) <= 32:
        stages = [("gz", "gy", "gx")]
    elif sizes["gx"] * sizes["gy"] <= 16:
        stages = [("gz",), ("gx", "gy")]
    else:
        stages = [("gz",), ("gx",), ("gy",)]
    return [group_offsets(sizes, s)[::-1] for s in stages]


def kernel(sizes, local, dens_hbm, mom_hbm, fuel_hbm, modes_hbm, early_hbm, back_hbm, late_hbm,
           drate, mrate, hrate,
           f, modes, early, back, late, edges, sides, ypack, zpack, ztile, stage_own, stage_got,
           load_sem, halo_send, halo_recv, stage_send, stage_recv):
    size_x, size_y, size_z = local
    rows = size_x * size_y
    rows_z = 2 * ROWS
    me = {a: lax.axis_index(a) for a in sizes}
    stages = plan(sizes)

    def at(offset):
        return {a: lax.rem(me[a] + o, sizes[a]) for a, o in offset.items()}

    own = pl.ds(REACH, size_x)
    loads = [
        pltpu.make_async_copy(src, dst, load_sem.at[i])
        for i, (src, dst) in enumerate([
            (dens_hbm, f.at[0, own]), (mom_hbm, f.at[1, own]), (early_hbm, early),
            (fuel_hbm, f.at[2, own]), (modes_hbm, modes), (late_hbm, late), (back_hbm, back),
        ])
    ]
    for copy in loads:
        copy.start()
    barrier = pltpu.get_barrier_semaphore()
    partners = [o for group in stages for o in group]
    for offset in partners:
        pl.semaphore_signal(barrier, inc=1, device_id=at(offset), device_id_type=MESH)

    row = lax.broadcasted_iota(jnp.int32, (ROWS, 2 * HALF), 0)
    lane = lax.broadcasted_iota(jnp.int32, (ROWS, 2 * HALF), 1)
    pair = lax.rem(lane, HALF)
    kx = lax.div(pair, WIDTH)
    ky = pair - kx * WIDTH
    turn = jnp.zeros((ROWS, 2 * HALF), jnp.float32)
    for k, axis, size in ((kx - KMAX, "gx", size_x), (ky - KMAX, "gy", size_y), (row, "gz", size_z)):
        count = k.astype(jnp.float32) * me[axis].astype(jnp.float32)
        part = count / sizes[axis]
        turn = turn + (part - jnp.floor(part))
    turn = turn - jnp.floor(turn + 0.5)
    cos_p = jnp.cos(2.0 * math.pi * turn)
    sin_p = jnp.sin(2.0 * math.pi * turn)
    sign = jnp.where(lane < HALF, -1.0, 1.0)
    sin_p = sign * sin_p

    loads[0].wait()
    loads[1].wait()
    loads[2].wait()
    flat = lambda i: f[i, own].reshape(rows, size_z)
    vel = flat(1) / flat(0)
    deep = 2 * rows_z
    table_xy = early[deep : deep + 4 * HALF]
    vel_both = jnp.concatenate(split(vel), 0)
    part = fold(dot_split(early[0:deep], vel_both, ((1,), (1,))))
    grid = fold(dot_split(jnp.concatenate(split(part), 0), table_xy, ((1,), (1,))))
    cube = grid[0:ROWS] + sign * pltpu.roll(grid[ROWS:], HALF, 1)
    cube = cos_p * cube + sin_p * pltpu.roll(cube, HALF, 1)
    stage_own[0] = cube

    def send_stage(s):
        base = sum(len(g) for g in stages[:s])
        copies = []
        for i, offset in enumerate(stages[s]):
            copy = pltpu.make_async_remote_copy(
                src_ref=stage_own.at[s], dst_ref=stage_got.at[base + i],
                send_sem=stage_send.at[base + i], recv_sem=stage_recv.at[base + i],
                device_id=at(offset), device_id_type=MESH)
            copy.start()
            copies.append(copy)
        return copies

    def sum_stage(s, copies):
        base = sum(len(g) for g in stages[:s])
        for copy in copies:
            copy.wait_recv()
        return tree_sum([stage_own[s]] + [stage_got[base + i] for i in range(len(copies))])

    pl.semaphore_wait(barrier, len(partners))
    pending = send_stage(0)
    started = list(pending)
    loads[3].wait()

    def send(src, dst, slot, axis, step):
        copy = pltpu.make_async_remote_copy(
            src_ref=src, dst_ref=dst, send_sem=halo_send.at[slot], recv_sem=halo_recv.at[slot],
            device_id=at({axis: step % sizes[axis]}), device_id_type=MESH)
        copy.start()
        return copy

    loads[5].wait()
    halos_x = [
        send(f.at[:, pl.ds(size_x, REACH)], f.at[:, pl.ds(0, REACH)], 0, "gx", 1),
        send(f.at[:, pl.ds(REACH, REACH)], f.at[:, pl.ds(size_x + REACH, REACH)], 1, "gx", -1),
    ]
    for i in range(2):
        ypack[i, :, 0:REACH] = f[1 + i, own, 0:REACH]
        ypack[i, :, REACH : 2 * REACH] = f[1 + i, own, size_y - REACH : size_y]
        zpack[i] = dot_nt(late[0:8], flat(1 + i))
    halos_y = [send(ypack, sides.at[0], 2, "gy", 1)]
    if sizes["gy"] > 2:
        halos_y.append(send(ypack, sides.at[1], 3, "gy", -1))
    halos_z = [send(zpack, ztile.at[0], 4, "gz", 1), send(zpack, ztile.at[1], 5, "gz", -1)]

    loads[4].wait()
    count = modes.shape[1]
    row_z = lax.broadcasted_iota(jnp.int32, (ROWS, count), 0)
    row_xy = lax.rem(lax.broadcasted_iota(jnp.int32, (2 * HALF, count), 0), HALF)
    code = (modes[0:1] + KMAX) * WIDTH + modes[1:2] + KMAX
    hits = [((row_z == modes[2:3]), (row_xy == code)),
            ((row_z == -modes[2:3]) & (row_z > 0), (row_xy == WIDTH * WIDTH - 1 - code))]
    chosen = sum(dot_nt(hz.astype(jnp.float32), hxy.astype(jnp.float32)) for hz, hxy in hits)

    lap = [dot_nn(flat(1 + i), late[24 : 24 + size_z]).reshape(size_x, size_y, size_z) for i in range(2)]
    outs = (drate, mrate, hrate)
    mrate[...] = lap[0]
    hrate[...] = lap[1]

    for s in range(1, len(stages)):
        stage_own[s] = sum_stage(s - 1, pending)
        pending = send_stage(s)
        started += pending

    for copy in halos_z:
        copy.wait_recv()
    for copy in halos_y:
        copy.wait_recv()
    for i in range(2):
        tile = jnp.concatenate([ztile[0, i], ztile[1, i]], 0)
        edges[i, :, 0:8] = sides[0, i]
        edges[i, :, 8 : 8 + size_y] = f[1 + i, own]
        edges[i, :, 8 + size_y : 16 + size_y] = sides[1 if sizes["gy"] > 2 else 0, i]
        total = outs[1 + i][...] + dot_tn(tile, late[8:24]).reshape(size_x, size_y, size_z)
        for offset, weight in enumerate(SECOND_COEFFS, 1):
            total = total + weight * (
                edges[i, :, 8 + offset : 8 + offset + size_y] + edges[i, :, 8 - offset : 8 - offset + size_y])
        outs[1 + i][...] = total

    for copy in halos_x:
        copy.wait_recv()
    def planes(x, offset):
        return x[REACH + offset : REACH + offset + size_x]

    def first_diff(x):
        total = None
        for offset, weight in enumerate(FIRST_COEFFS, 1):
            term = weight * (planes(x, offset) - planes(x, -offset))
            total = term if total is None else total + term
        return total

    def second_diff(x):
        return tree_sum([w * (planes(x, o) + planes(x, -o)) for o, w in enumerate(SECOND_COEFFS, 1)])

    mom = f[1]
    dens = f[0]
    fuel = f[2]
    vel_pad = mom / dens
    drate[...] = -first_diff(mom)
    mid_fuel = planes(fuel, 0)
    hrate[...] = (DIFFUSIVITY * (hrate[...] + second_diff(fuel)) - first_diff(fuel * vel_pad)
                  - mid_fuel * jnp.exp(-ACTIVATION * mid_fuel / planes(dens, 0)))
    mrate[...] = VISCOSITY * (mrate[...] + second_diff(mom)) - first_diff(mom * vel_pad + dens)

    loads[6].wait()
    ncell = float(rows * size_z * math.prod(sizes.values()))
    cube = sum_stage(len(stages) - 1, pending)
    coef = cube / ncell
    picked = chosen * coef
    energy = jnp.sum(jnp.sum(picked * coef, axis=1, keepdims=True), axis=0, keepdims=True)
    scale = 2.0 * FORCE_POWER / (energy + ENERGY_EPS)
    local_coef = cos_p * picked - sin_p * pltpu.roll(picked, HALF, 1)
    both = jnp.concatenate([local_coef, -sign * pltpu.roll(local_coef, HALF, 1)], 0)
    wave = fold(dot_split(jnp.concatenate(split(both), 0), back[...], ((1,), (0,))))
    high, rest = split(wave)
    waves = jnp.concatenate([high, rest, high, rest], 0).T
    low = dot_split(waves, early[deep + 4 * HALF : deep + 4 * HALF + 4 * rows_z], ((1,), (0,)))
    low = low.reshape(size_x, size_y, size_z)
    mrate[...] = mrate[...] + f[0, own] * (low * scale.reshape(1, 1, 1))
    for copy in started + halos_x + halos_y + halos_z:
        copy.wait_send()


def write_out(*refs):
    count = len(refs) // 2
    copies = [pltpu.make_async_copy(refs[i], refs[count + i], refs[-1].at[i]) for i in range(count)]
    for copy in copies:
        copy.start()
    for copy in copies:
        copy.wait()


def solution(mesh):
    sizes = {a: mesh.shape[a] for a in ("gx", "gy", "gz")}

    def per_device(density, momentum, hydrogen, forced_modes):
        local = density.shape
        size_x, size_y, size_z = local
        rows = size_x * size_y
        full = (size_x * sizes["gx"], size_y * sizes["gy"], size_z * sizes["gz"])
        early, back, late = tables(local, full)
        modes = forced_modes.T
        stages = plan(sizes)
        messages = sum(len(g) for g in stages)
        any_spec = pl.BlockSpec(memory_space=pl.ANY)
        f32 = jnp.float32
        rates = pl.pallas_call(
            functools.partial(kernel, sizes, local),
            out_shape=[pltpu.VMEM(local, f32)] * 3,
            in_specs=[any_spec] * 7,
            out_specs=[pl.BlockSpec(memory_space=pltpu.VMEM)] * 3,
            scratch_shapes=[
                pltpu.VMEM((3, size_x + 2 * REACH, size_y, size_z), f32),
                pltpu.VMEM(modes.shape, jnp.int32),
                pltpu.VMEM(early.shape, jnp.bfloat16),
                pltpu.VMEM(back.shape, jnp.bfloat16),
                pltpu.VMEM(late.shape, f32),
                pltpu.VMEM((2, size_x, size_y + 16, size_z), f32),
                pltpu.VMEM((2, 2, size_x, 8, size_z), f32),
                pltpu.VMEM((2, size_x, 8, size_z), f32),
                pltpu.VMEM((2, 8, rows), f32),
                pltpu.VMEM((2, 2, 8, rows), f32),
                pltpu.VMEM((len(stages), ROWS, 2 * HALF), f32),
                pltpu.VMEM((messages, ROWS, 2 * HALF), f32),
                pltpu.SemaphoreType.DMA((7,)),
                pltpu.SemaphoreType.DMA((6,)),
                pltpu.SemaphoreType.DMA((6,)),
                pltpu.SemaphoreType.DMA((messages,)),
                pltpu.SemaphoreType.DMA((messages,)),
            ],
            compiler_params=pltpu.CompilerParams(collective_id=0, has_side_effects=True),
            name="flame",
        )(density, momentum, hydrogen, modes, jnp.asarray(early), jnp.asarray(back), jnp.asarray(late))
        return tuple(pl.pallas_call(
            write_out,
            out_shape=[jax.ShapeDtypeStruct(local, f32)] * 3,
            in_specs=[pl.BlockSpec(memory_space=pltpu.VMEM)] * 3,
            out_specs=[any_spec] * 3,
            scratch_shapes=[pltpu.SemaphoreType.DMA((3,))],
            name="write",
        )(*[pltpu.with_memory_space_constraint(r, pltpu.VMEM) for r in rates]))

    in_specs = (P("gx", "gy", "gz"), P("gx", "gy", "gz"), P("gx", "gy", "gz"), P())
    out_specs = (P("gx", "gy", "gz"), P("gx", "gy", "gz"), P("gx", "gy", "gz"))
    return jax.shard_map(
        per_device, mesh=mesh, in_specs=in_specs, out_specs=out_specs, check_vma=False
    )
```

```python
import functools
import math

import jax
import jax.numpy as jnp
import numpy as np
from jax import lax
from jax.experimental import pallas as pl
from jax.experimental.pallas import tpu as pltpu
from jax.sharding import PartitionSpec as P

KMAX = 3
WIDTH = 2 * KMAX + 1
HALF = 64
ROWS = KMAX + 1
REACH = 4

FIRST_COEFFS = (0.8, -0.2, 4.0 / 105.0, -1.0 / 280.0)
SECOND_COEFFS = (1.6, -0.2, 8.0 / 315.0, -1.0 / 560.0)
CENTRE_COEFF = -205.0 / 72.0
VISCOSITY = 0.3
DIFFUSIVITY = 1.5
FORCE_POWER = 0.3
ENERGY_EPS = 1e-06
ACTIVATION = 2.0
HIGHEST = lax.Precision.HIGHEST
MESH = pl.DeviceIdType.MESH


def tables(local, full):
    size_x, size_y, size_z = local
    full_x, full_y, full_z = full
    k = np.arange(-KMAX, KMAX + 1)
    ang_z = 2.0 * np.pi * (k[:, None] * np.arange(size_z)[None, :]) / full_z
    trig_z = np.zeros((2 * ROWS, size_z))
    trig_z[:ROWS] = np.cos(ang_z[KMAX:])
    trig_z[ROWS:] = np.sin(ang_z[KMAX:])
    ax = k[:, None] * np.arange(size_x)[None, :] / full_x
    ay = k[:, None] * np.arange(size_y)[None, :] / full_y
    ang = 2.0 * np.pi * (ax[:, None, :, None] + ay[None, :, None, :])
    ang = ang.reshape(WIDTH * WIDTH, size_x * size_y)
    trig_xy = np.zeros((2 * HALF, size_x * size_y))
    trig_xy[: WIDTH * WIDTH] = np.cos(ang)
    trig_xy[HALF : HALF + WIDTH * WIDTH] = np.sin(ang)
    edge = np.zeros((8, size_z))
    for j in range(REACH):
        edge[j, j] = 1.0
        edge[REACH + j, size_z - REACH + j] = 1.0
    band = np.zeros((size_z, size_z))
    halo = np.zeros((16, size_z))
    for z in range(size_z):
        band[z, z] = 3.0 * CENTRE_COEFF
        for offset, weight in enumerate(SECOND_COEFFS, 1):
            for q in (z - offset, z + offset):
                if 0 <= q < size_z:
                    band[q, z] = weight
                elif q < 0:
                    halo[8 + q, z] = weight
                else:
                    halo[8 + q - size_z, z] = weight
    z_high, z_low = split_host(trig_z)
    xy_high, xy_low = split_host(trig_xy)
    early = np.concatenate([z_high, z_low, xy_high, xy_low, z_high, z_high, z_low, z_low], 0)
    back = np.concatenate([xy_high, xy_low], 1)
    late = np.concatenate([edge, halo, band], 0).astype(np.float32)
    return early, back, late


def split_host(table):
    high = table.astype(np.float32).astype(jnp.bfloat16)
    low = (table - high.astype(np.float64)).astype(np.float32).astype(jnp.bfloat16)
    return high, low


def split(x):
    high = x.astype(jnp.bfloat16).astype(jnp.float32)
    return high, x - high


def dot_split(a, b, contract):
    return lax.dot_general(a.astype(jnp.bfloat16), b.astype(jnp.bfloat16), (contract, ((), ())),
                           preferred_element_type=jnp.float32)


def fold(x):
    rows, lanes = x.shape
    x = x[: rows // 2] + x[rows // 2 :]
    return x[:, : lanes // 2] + x[:, lanes // 2 :]


def dot_nt(a, b):
    return lax.dot_general(a, b, (((1,), (1,)), ((), ())), precision=HIGHEST, preferred_element_type=jnp.float32)


def dot_nn(a, b):
    return lax.dot_general(a, b, (((1,), (0,)), ((), ())), precision=HIGHEST, preferred_element_type=jnp.float32)


def dot_tn(a, b):
    return lax.dot_general(a, b, (((0,), (0,)), ((), ())), precision=HIGHEST, preferred_element_type=jnp.float32)


def group_offsets(sizes, axes):
    offsets = [{}]
    for axis in axes:
        offsets = [{**o, axis: s} for o in offsets for s in range(sizes[axis])]
    return [o for o in offsets if any(o.values())]


def tree_sum(parts):
    parts = list(parts)
    while len(parts) > 1:
        parts = [sum(parts[i : i + 2][1:], parts[i]) for i in range(0, len(parts), 2)]
    return parts[0]


def plan(sizes):
    if math.prod(sizes.values()) <= 32:
        stages = [("gz", "gy", "gx")]
    elif sizes["gx"] * sizes["gy"] <= 16:
        stages = [("gz",), ("gx", "gy")]
    else:
        stages = [("gz",), ("gx",), ("gy",)]
    return [group_offsets(sizes, s)[::-1] for s in stages]


def kernel(sizes, local, dens_hbm, mom_hbm, fuel_hbm, modes_hbm, early_hbm, back_hbm, late_hbm,
           drate, mrate, hrate,
           f, modes, early, back, late, edges, sides, ypack, zpack, ztile, stage_own, stage_got,
           load_sem, halo_send, halo_recv, stage_send, stage_recv):
    size_x, size_y, size_z = local
    rows = size_x * size_y
    rows_z = 2 * ROWS
    me = {a: lax.axis_index(a) for a in sizes}
    stages = plan(sizes)

    def at(offset):
        return {a: lax.rem(me[a] + o, sizes[a]) for a, o in offset.items()}

    own = pl.ds(REACH, size_x)
    loads = [
        pltpu.make_async_copy(src, dst, load_sem.at[i])
        for i, (src, dst) in enumerate([
            (dens_hbm, f.at[0, own]), (mom_hbm, f.at[1, own]), (early_hbm, early),
            (fuel_hbm, f.at[2, own]), (modes_hbm, modes), (late_hbm, late), (back_hbm, back),
        ])
    ]
    for copy in loads:
        copy.start()
    barrier = pltpu.get_barrier_semaphore()
    partners = [o for group in stages for o in group]
    for offset in partners:
        pl.semaphore_signal(barrier, inc=1, device_id=at(offset), device_id_type=MESH)

    row = lax.broadcasted_iota(jnp.int32, (ROWS, 2 * HALF), 0)
    lane = lax.broadcasted_iota(jnp.int32, (ROWS, 2 * HALF), 1)
    pair = lax.rem(lane, HALF)
    kx = lax.div(pair, WIDTH)
    ky = pair - kx * WIDTH
    turn = jnp.zeros((ROWS, 2 * HALF), jnp.float32)
    for k, axis, size in ((kx - KMAX, "gx", size_x), (ky - KMAX, "gy", size_y), (row, "gz", size_z)):
        count = k.astype(jnp.float32) * me[axis].astype(jnp.float32)
        part = count / sizes[axis]
        turn = turn + (part - jnp.floor(part))
    turn = turn - jnp.floor(turn + 0.5)
    cos_p = jnp.cos(2.0 * math.pi * turn)
    sin_p = jnp.sin(2.0 * math.pi * turn)
    sign = jnp.where(lane < HALF, -1.0, 1.0)
    sin_p = sign * sin_p

    loads[0].wait()
    loads[1].wait()
    loads[2].wait()
    flat = lambda i: f[i, own].reshape(rows, size_z)
    vel = flat(1) / flat(0)
    deep = 2 * rows_z
    table_xy = early[deep : deep + 4 * HALF]
    vel_both = jnp.concatenate(split(vel), 0)
    part = fold(dot_split(early[0:deep], vel_both, ((1,), (1,))))
    grid = fold(dot_split(jnp.concatenate(split(part), 0), table_xy, ((1,), (1,))))
    cube = grid[0:ROWS] + sign * pltpu.roll(grid[ROWS:], HALF, 1)
    cube = cos_p * cube + sin_p * pltpu.roll(cube, HALF, 1)
    stage_own[0] = cube

    def span(s):
        base = sum(len(g) for g in stages[:s])
        return pl.ds(base, len(stages[s]))

    def send_stage(s):
        base = sum(len(g) for g in stages[:s])
        for i, offset in enumerate(stages[s]):
            pltpu.make_async_remote_copy(
                src_ref=stage_own.at[s], dst_ref=stage_got.at[base + i],
                send_sem=stage_send.at[s], recv_sem=stage_recv.at[s],
                device_id=at(offset), device_id_type=MESH).start()

    def wait_stage(s, sem):
        got = stage_got.at[span(s)]
        pltpu.make_async_copy(got, got, sem.at[s]).wait()

    def sum_stage(s):
        base = sum(len(g) for g in stages[:s])
        wait_stage(s, stage_recv)
        return tree_sum([stage_own[s]] + [stage_got[base + i] for i in range(len(stages[s]))])

    pl.semaphore_wait(barrier, len(partners))
    send_stage(0)
    loads[3].wait()

    def send(src, dst, slot, axis, step):
        copy = pltpu.make_async_remote_copy(
            src_ref=src, dst_ref=dst, send_sem=halo_send.at[slot], recv_sem=halo_recv.at[slot],
            device_id=at({axis: step % sizes[axis]}), device_id_type=MESH)
        copy.start()
        return copy

    loads[5].wait()
    halos_x = [
        send(f.at[:, pl.ds(size_x, REACH)], f.at[:, pl.ds(0, REACH)], 0, "gx", 1),
        send(f.at[:, pl.ds(REACH, REACH)], f.at[:, pl.ds(size_x + REACH, REACH)], 1, "gx", -1),
    ]
    for i in range(2):
        ypack[i, :, 0:REACH] = f[1 + i, own, 0:REACH]
        ypack[i, :, REACH : 2 * REACH] = f[1 + i, own, size_y - REACH : size_y]
        zpack[i] = dot_nt(late[0:8], flat(1 + i))
    halos_y = [send(ypack, sides.at[0], 2, "gy", 1)]
    if sizes["gy"] > 2:
        halos_y.append(send(ypack, sides.at[1], 3, "gy", -1))
    halos_z = [send(zpack, ztile.at[0], 4, "gz", 1), send(zpack, ztile.at[1], 5, "gz", -1)]

    loads[4].wait()
    count = modes.shape[1]
    row_z = lax.broadcasted_iota(jnp.int32, (ROWS, count), 0)
    row_xy = lax.rem(lax.broadcasted_iota(jnp.int32, (2 * HALF, count), 0), HALF)
    code = (modes[0:1] + KMAX) * WIDTH + modes[1:2] + KMAX
    hits = [((row_z == modes[2:3]), (row_xy == code)),
            ((row_z == -modes[2:3]) & (row_z > 0), (row_xy == WIDTH * WIDTH - 1 - code))]
    chosen = sum(dot_nt(hz.astype(jnp.float32), hxy.astype(jnp.float32)) for hz, hxy in hits)

    lap = [dot_nn(flat(1 + i), late[24 : 24 + size_z]).reshape(size_x, size_y, size_z) for i in range(2)]
    outs = (drate, mrate, hrate)
    mrate[...] = lap[0]
    hrate[...] = lap[1]

    for s in range(1, len(stages)):
        stage_own[s] = sum_stage(s - 1)
        send_stage(s)

    for copy in halos_z:
        copy.wait_recv()
    for copy in halos_y:
        copy.wait_recv()
    for i in range(2):
        tile = jnp.concatenate([ztile[0, i], ztile[1, i]], 0)
        edges[i, :, 0:8] = sides[0, i]
        edges[i, :, 8 : 8 + size_y] = f[1 + i, own]
        edges[i, :, 8 + size_y : 16 + size_y] = sides[1 if sizes["gy"] > 2 else 0, i]
        total = outs[1 + i][...] + dot_tn(tile, late[8:24]).reshape(size_x, size_y, size_z)
        for offset, weight in enumerate(SECOND_COEFFS, 1):
            total = total + weight * (
                edges[i, :, 8 + offset : 8 + offset + size_y] + edges[i, :, 8 - offset : 8 - offset + size_y])
        outs[1 + i][...] = total

    for copy in halos_x:
        copy.wait_recv()
    def planes(x, offset):
        return x[REACH + offset : REACH + offset + size_x]

    def first_diff(x):
        total = None
        for offset, weight in enumerate(FIRST_COEFFS, 1):
            term = weight * (planes(x, offset) - planes(x, -offset))
            total = term if total is None else total + term
        return total

    def second_diff(x):
        return tree_sum([w * (planes(x, o) + planes(x, -o)) for o, w in enumerate(SECOND_COEFFS, 1)])

    mom = f[1]
    dens = f[0]
    fuel = f[2]
    vel_pad = mom / dens
    drate[...] = -first_diff(mom)
    mid_fuel = planes(fuel, 0)
    hrate[...] = (DIFFUSIVITY * (hrate[...] + second_diff(fuel)) - first_diff(fuel * vel_pad)
                  - mid_fuel * jnp.exp(-ACTIVATION * mid_fuel / planes(dens, 0)))
    mrate[...] = VISCOSITY * (mrate[...] + second_diff(mom)) - first_diff(mom * vel_pad + dens)

    loads[6].wait()
    ncell = float(rows * size_z * math.prod(sizes.values()))
    cube = sum_stage(len(stages) - 1)
    coef = cube / ncell
    picked = chosen * coef
    energy = jnp.sum(jnp.sum(picked * coef, axis=1, keepdims=True), axis=0, keepdims=True)
    scale = 2.0 * FORCE_POWER / (energy + ENERGY_EPS)
    local_coef = cos_p * picked - sin_p * pltpu.roll(picked, HALF, 1)
    both = jnp.concatenate([local_coef, -sign * pltpu.roll(local_coef, HALF, 1)], 0)
    wave = fold(dot_split(jnp.concatenate(split(both), 0), back[...], ((1,), (0,))))
    high, rest = split(wave)
    waves = jnp.concatenate([high, rest, high, rest], 0).T
    low = dot_split(waves, early[deep + 4 * HALF : deep + 4 * HALF + 4 * rows_z], ((1,), (0,)))
    low = low.reshape(size_x, size_y, size_z)
    mrate[...] = mrate[...] + f[0, own] * (low * scale.reshape(1, 1, 1))
    for copy in halos_x + halos_y + halos_z:
        copy.wait_send()
    for s in range(len(stages)):
        wait_stage(s, stage_send)


def write_out(*refs):
    count = len(refs) // 2
    copies = [pltpu.make_async_copy(refs[i], refs[count + i], refs[-1].at[i]) for i in range(count)]
    for copy in copies:
        copy.start()
    for copy in copies:
        copy.wait()


def solution(mesh):
    sizes = {a: mesh.shape[a] for a in ("gx", "gy", "gz")}

    def per_device(density, momentum, hydrogen, forced_modes):
        local = density.shape
        size_x, size_y, size_z = local
        rows = size_x * size_y
        full = (size_x * sizes["gx"], size_y * sizes["gy"], size_z * sizes["gz"])
        early, back, late = tables(local, full)
        modes = forced_modes.T
        stages = plan(sizes)
        messages = sum(len(g) for g in stages)
        any_spec = pl.BlockSpec(memory_space=pl.ANY)
        f32 = jnp.float32
        rates = pl.pallas_call(
            functools.partial(kernel, sizes, local),
            out_shape=[pltpu.VMEM(local, f32)] * 3,
            in_specs=[any_spec] * 7,
            out_specs=[pl.BlockSpec(memory_space=pltpu.VMEM)] * 3,
            scratch_shapes=[
                pltpu.VMEM((3, size_x + 2 * REACH, size_y, size_z), f32),
                pltpu.VMEM(modes.shape, jnp.int32),
                pltpu.VMEM(early.shape, jnp.bfloat16),
                pltpu.VMEM(back.shape, jnp.bfloat16),
                pltpu.VMEM(late.shape, f32),
                pltpu.VMEM((2, size_x, size_y + 16, size_z), f32),
                pltpu.VMEM((2, 2, size_x, 8, size_z), f32),
                pltpu.VMEM((2, size_x, 8, size_z), f32),
                pltpu.VMEM((2, 8, rows), f32),
                pltpu.VMEM((2, 2, 8, rows), f32),
                pltpu.VMEM((len(stages), ROWS, 2 * HALF), f32),
                pltpu.VMEM((messages, ROWS, 2 * HALF), f32),
                pltpu.SemaphoreType.DMA((7,)),
                pltpu.SemaphoreType.DMA((6,)),
                pltpu.SemaphoreType.DMA((6,)),
                pltpu.SemaphoreType.DMA((len(stages),)),
                pltpu.SemaphoreType.DMA((len(stages),)),
            ],
            compiler_params=pltpu.CompilerParams(collective_id=0, has_side_effects=True),
            name="flame",
        )(density, momentum, hydrogen, modes, jnp.asarray(early), jnp.asarray(back), jnp.asarray(late))
        return tuple(pl.pallas_call(
            write_out,
            out_shape=[jax.ShapeDtypeStruct(local, f32)] * 3,
            in_specs=[pl.BlockSpec(memory_space=pltpu.VMEM)] * 3,
            out_specs=[any_spec] * 3,
            scratch_shapes=[pltpu.SemaphoreType.DMA((3,))],
            name="write",
        )(*[pltpu.with_memory_space_constraint(r, pltpu.VMEM) for r in rates]))

    in_specs = (P("gx", "gy", "gz"), P("gx", "gy", "gz"), P("gx", "gy", "gz"), P())
    out_specs = (P("gx", "gy", "gz"), P("gx", "gy", "gz"), P("gx", "gy", "gz"))
    return jax.shard_map(
        per_device, mesh=mesh, in_specs=in_specs, out_specs=out_specs, check_vma=False
    )
```

```python
import functools
import math

import jax
import jax.numpy as jnp
import numpy as np
from jax import lax
from jax.experimental import pallas as pl
from jax.experimental.pallas import tpu as pltpu
from jax.sharding import PartitionSpec as P

KMAX = 3
WIDTH = 2 * KMAX + 1
HALF = 64
ROWS = KMAX + 1
REACH = 4

FIRST_COEFFS = (0.8, -0.2, 4.0 / 105.0, -1.0 / 280.0)
SECOND_COEFFS = (1.6, -0.2, 8.0 / 315.0, -1.0 / 560.0)
CENTRE_COEFF = -205.0 / 72.0
VISCOSITY = 0.3
DIFFUSIVITY = 1.5
FORCE_POWER = 0.3
ENERGY_EPS = 1e-06
ACTIVATION = 2.0
HIGHEST = lax.Precision.HIGHEST
MESH = pl.DeviceIdType.MESH


def tables(local, full):
    size_x, size_y, size_z = local
    full_x, full_y, full_z = full
    k = np.arange(-KMAX, KMAX + 1)
    ang_z = 2.0 * np.pi * (k[:, None] * np.arange(size_z)[None, :]) / full_z
    trig_z = np.zeros((2 * ROWS, size_z))
    trig_z[:ROWS] = np.cos(ang_z[KMAX:])
    trig_z[ROWS:] = np.sin(ang_z[KMAX:])
    ax = k[:, None] * np.arange(size_x)[None, :] / full_x
    ay = k[:, None] * np.arange(size_y)[None, :] / full_y
    ang = 2.0 * np.pi * (ax[:, None, :, None] + ay[None, :, None, :])
    ang = ang.reshape(WIDTH * WIDTH, size_x * size_y)
    trig_xy = np.zeros((2 * HALF, size_x * size_y))
    trig_xy[: WIDTH * WIDTH] = np.cos(ang)
    trig_xy[HALF : HALF + WIDTH * WIDTH] = np.sin(ang)
    edge = np.zeros((8, size_z))
    for j in range(REACH):
        edge[j, j] = 1.0
        edge[REACH + j, size_z - REACH + j] = 1.0
    band = np.zeros((size_z, size_z))
    halo = np.zeros((16, size_z))
    for z in range(size_z):
        band[z, z] = 3.0 * CENTRE_COEFF
        for offset, weight in enumerate(SECOND_COEFFS, 1):
            for q in (z - offset, z + offset):
                if 0 <= q < size_z:
                    band[q, z] = weight
                elif q < 0:
                    halo[8 + q, z] = weight
                else:
                    halo[8 + q - size_z, z] = weight
    z_high, z_low = split_host(trig_z)
    xy_high, xy_low = split_host(trig_xy)
    early = np.concatenate([z_high, z_low, xy_high, xy_low, z_high, z_high, z_low, z_low,
                            split_host(np.concatenate([edge, np.zeros_like(edge)], 0))[0]], 0)
    back = np.concatenate([xy_high, xy_low], 1)
    late = np.concatenate([halo, band], 0).astype(np.float32)
    return early, back, late


def split_host(table):
    high = table.astype(np.float32).astype(jnp.bfloat16)
    low = (table - high.astype(np.float64)).astype(np.float32).astype(jnp.bfloat16)
    return high, low


def split(x):
    high = x.astype(jnp.bfloat16).astype(jnp.float32)
    return high, x - high


def dot_split(a, b, contract):
    return lax.dot_general(a.astype(jnp.bfloat16), b.astype(jnp.bfloat16), (contract, ((), ())),
                           preferred_element_type=jnp.float32)


def fold(x):
    rows, lanes = x.shape
    x = x[: rows // 2] + x[rows // 2 :]
    return x[:, : lanes // 2] + x[:, lanes // 2 :]


def dot_nt(a, b):
    return lax.dot_general(a, b, (((1,), (1,)), ((), ())), precision=HIGHEST, preferred_element_type=jnp.float32)


def dot_nn(a, b):
    return lax.dot_general(a, b, (((1,), (0,)), ((), ())), precision=HIGHEST, preferred_element_type=jnp.float32)


def dot_tn(a, b):
    return lax.dot_general(a, b, (((0,), (0,)), ((), ())), precision=HIGHEST, preferred_element_type=jnp.float32)


def group_offsets(sizes, axes):
    offsets = [{}]
    for axis in axes:
        offsets = [{**o, axis: s} for o in offsets for s in range(sizes[axis])]
    return [o for o in offsets if any(o.values())]


def tree_sum(parts):
    parts = list(parts)
    while len(parts) > 1:
        parts = [sum(parts[i : i + 2][1:], parts[i]) for i in range(0, len(parts), 2)]
    return parts[0]


def plan(sizes):
    if math.prod(sizes.values()) <= 32:
        stages = [("gz", "gy", "gx")]
    elif sizes["gx"] * sizes["gy"] <= 16:
        stages = [("gz",), ("gx", "gy")]
    else:
        stages = [("gz",), ("gx",), ("gy",)]
    return [group_offsets(sizes, s)[::-1] for s in stages]


def kernel(sizes, local, dens_hbm, mom_hbm, fuel_hbm, modes_hbm, early_hbm, back_hbm, late_hbm,
           drate, mrate, hrate,
           f, modes, early, back, late, edges, sides, ypack, zpack, ztile, stage_own, stage_got,
           load_sem, halo_send, halo_recv, stage_send, stage_recv):
    size_x, size_y, size_z = local
    rows = size_x * size_y
    rows_z = 2 * ROWS
    me = {a: lax.axis_index(a) for a in sizes}
    stages = plan(sizes)

    def at(offset):
        return {a: lax.rem(me[a] + o, sizes[a]) for a, o in offset.items()}

    own = pl.ds(REACH, size_x)
    loads = [
        pltpu.make_async_copy(src, dst, load_sem.at[i])
        for i, (src, dst) in enumerate([
            (dens_hbm, f.at[0, own]), (mom_hbm, f.at[1, own]), (early_hbm, early),
            (fuel_hbm, f.at[2, own]), (modes_hbm, modes), (late_hbm, late), (back_hbm, back),
        ])
    ]
    for copy in loads:
        copy.start()
    barrier = pltpu.get_barrier_semaphore()
    partners = [o for group in stages for o in group]
    for offset in partners:
        pl.semaphore_signal(barrier, inc=1, device_id=at(offset), device_id_type=MESH)

    row = lax.broadcasted_iota(jnp.int32, (ROWS, 2 * HALF), 0)
    lane = lax.broadcasted_iota(jnp.int32, (ROWS, 2 * HALF), 1)
    pair = lax.rem(lane, HALF)
    kx = lax.div(pair, WIDTH)
    ky = pair - kx * WIDTH
    turn = jnp.zeros((ROWS, 2 * HALF), jnp.float32)
    for k, axis, size in ((kx - KMAX, "gx", size_x), (ky - KMAX, "gy", size_y), (row, "gz", size_z)):
        count = k.astype(jnp.float32) * me[axis].astype(jnp.float32)
        part = count / sizes[axis]
        turn = turn + (part - jnp.floor(part))
    turn = turn - jnp.floor(turn + 0.5)
    cos_p = jnp.cos(2.0 * math.pi * turn)
    sin_p = jnp.sin(2.0 * math.pi * turn)
    sign = jnp.where(lane < HALF, -1.0, 1.0)
    sin_p = sign * sin_p

    loads[0].wait()
    loads[1].wait()
    loads[2].wait()
    flat = lambda i: f[i, own].reshape(rows, size_z)
    vel = flat(1) / flat(0)
    deep = 2 * rows_z
    table_xy = early[deep : deep + 4 * HALF]
    vel_both = jnp.concatenate(split(vel), 0)
    part = fold(dot_split(early[0:deep], vel_both, ((1,), (1,))))
    grid = fold(dot_split(jnp.concatenate(split(part), 0), table_xy, ((1,), (1,))))
    cube = grid[0:ROWS] + sign * pltpu.roll(grid[ROWS:], HALF, 1)
    cube = cos_p * cube + sin_p * pltpu.roll(cube, HALF, 1)
    stage_own[0] = cube

    def span(s):
        base = sum(len(g) for g in stages[:s])
        return pl.ds(base, len(stages[s]))

    def send_stage(s):
        base = sum(len(g) for g in stages[:s])
        for i, offset in enumerate(stages[s]):
            pltpu.make_async_remote_copy(
                src_ref=stage_own.at[s], dst_ref=stage_got.at[base + i],
                send_sem=stage_send.at[s], recv_sem=stage_recv.at[s],
                device_id=at(offset), device_id_type=MESH).start()

    def wait_stage(s, sem):
        got = stage_got.at[span(s)]
        pltpu.make_async_copy(got, got, sem.at[s]).wait()

    def sum_stage(s):
        base = sum(len(g) for g in stages[:s])
        wait_stage(s, stage_recv)
        return tree_sum([stage_own[s]] + [stage_got[base + i] for i in range(len(stages[s]))])

    loads[3].wait()
    pieces = []
    for i in range(2):
        ypack[i, :, 0:REACH] = f[1 + i, own, 0:REACH]
        ypack[i, :, REACH : 2 * REACH] = f[1 + i, own, size_y - REACH : size_y]
        high, rest = split(flat(1 + i))
        pieces += [high, *split(rest)]
    edge_at = deep + 4 * HALF + 4 * rows_z
    ends = dot_split(early[edge_at : edge_at + 16], jnp.concatenate(pieces, 0), ((1,), (1,)))[0:8]
    for i in range(2):
        zpack[i] = tree_sum([ends[:, (3 * i + j) * rows : (3 * i + j + 1) * rows] for j in range(3)])

    pl.semaphore_wait(barrier, len(partners))
    send_stage(0)

    def send(src, dst, slot, axis, step):
        copy = pltpu.make_async_remote_copy(
            src_ref=src, dst_ref=dst, send_sem=halo_send.at[slot], recv_sem=halo_recv.at[slot],
            device_id=at({axis: step % sizes[axis]}), device_id_type=MESH)
        copy.start()
        return copy

    halos_x = [
        send(f.at[:, pl.ds(size_x, REACH)], f.at[:, pl.ds(0, REACH)], 0, "gx", 1),
        send(f.at[:, pl.ds(REACH, REACH)], f.at[:, pl.ds(size_x + REACH, REACH)], 1, "gx", -1),
    ]
    halos_y = [send(ypack, sides.at[0], 2, "gy", 1)]
    if sizes["gy"] > 2:
        halos_y.append(send(ypack, sides.at[1], 3, "gy", -1))
    halos_z = [send(zpack, ztile.at[0], 4, "gz", 1), send(zpack, ztile.at[1], 5, "gz", -1)]

    loads[4].wait()
    count = modes.shape[1]
    row_z = lax.broadcasted_iota(jnp.int32, (ROWS, count), 0)
    row_xy = lax.rem(lax.broadcasted_iota(jnp.int32, (2 * HALF, count), 0), HALF)
    code = (modes[0:1] + KMAX) * WIDTH + modes[1:2] + KMAX
    hits = [((row_z == modes[2:3]), (row_xy == code)),
            ((row_z == -modes[2:3]) & (row_z > 0), (row_xy == WIDTH * WIDTH - 1 - code))]
    chosen = sum(dot_nt(hz.astype(jnp.float32), hxy.astype(jnp.float32)) for hz, hxy in hits)

    loads[5].wait()
    lap = [dot_nn(flat(1 + i), late[16 : 16 + size_z]).reshape(size_x, size_y, size_z) for i in range(2)]
    outs = (drate, mrate, hrate)
    mrate[...] = lap[0]
    hrate[...] = lap[1]

    for s in range(1, len(stages)):
        stage_own[s] = sum_stage(s - 1)
        send_stage(s)

    for copy in halos_z:
        copy.wait_recv()
    for copy in halos_y:
        copy.wait_recv()
    for i in range(2):
        tile = jnp.concatenate([ztile[0, i], ztile[1, i]], 0)
        edges[i, :, 0:8] = sides[0, i]
        edges[i, :, 8 : 8 + size_y] = f[1 + i, own]
        edges[i, :, 8 + size_y : 16 + size_y] = sides[1 if sizes["gy"] > 2 else 0, i]
        total = outs[1 + i][...] + dot_tn(tile, late[0:16]).reshape(size_x, size_y, size_z)
        for offset, weight in enumerate(SECOND_COEFFS, 1):
            total = total + weight * (
                edges[i, :, 8 + offset : 8 + offset + size_y] + edges[i, :, 8 - offset : 8 - offset + size_y])
        outs[1 + i][...] = total

    for copy in halos_x:
        copy.wait_recv()
    def planes(x, offset):
        return x[REACH + offset : REACH + offset + size_x]

    def first_diff(x):
        total = None
        for offset, weight in enumerate(FIRST_COEFFS, 1):
            term = weight * (planes(x, offset) - planes(x, -offset))
            total = term if total is None else total + term
        return total

    def second_diff(x):
        return tree_sum([w * (planes(x, o) + planes(x, -o)) for o, w in enumerate(SECOND_COEFFS, 1)])

    mom = f[1]
    dens = f[0]
    fuel = f[2]
    vel_pad = mom / dens
    drate[...] = -first_diff(mom)
    mid_fuel = planes(fuel, 0)
    hrate[...] = (DIFFUSIVITY * (hrate[...] + second_diff(fuel)) - first_diff(fuel * vel_pad)
                  - mid_fuel * jnp.exp(-ACTIVATION * mid_fuel / planes(dens, 0)))
    mrate[...] = VISCOSITY * (mrate[...] + second_diff(mom)) - first_diff(mom * vel_pad + dens)

    loads[6].wait()
    ncell = float(rows * size_z * math.prod(sizes.values()))
    cube = sum_stage(len(stages) - 1)
    coef = cube / ncell
    picked = chosen * coef
    energy = jnp.sum(jnp.sum(picked * coef, axis=1, keepdims=True), axis=0, keepdims=True)
    scale = 2.0 * FORCE_POWER / (energy + ENERGY_EPS)
    local_coef = cos_p * picked - sin_p * pltpu.roll(picked, HALF, 1)
    both = jnp.concatenate([local_coef, -sign * pltpu.roll(local_coef, HALF, 1)], 0)
    wave = fold(dot_split(jnp.concatenate(split(both), 0), back[...], ((1,), (0,))))
    high, rest = split(wave)
    waves = jnp.concatenate([high, rest, high, rest], 0).T
    low = dot_split(waves, early[deep + 4 * HALF : deep + 4 * HALF + 4 * rows_z], ((1,), (0,)))
    low = low.reshape(size_x, size_y, size_z)
    mrate[...] = mrate[...] + f[0, own] * (low * scale.reshape(1, 1, 1))
    for copy in halos_x + halos_y + halos_z:
        copy.wait_send()
    for s in range(len(stages)):
        wait_stage(s, stage_send)


def write_out(*refs):
    count = len(refs) // 2
    copies = [pltpu.make_async_copy(refs[i], refs[count + i], refs[-1].at[i]) for i in range(count)]
    for copy in copies:
        copy.start()
    for copy in copies:
        copy.wait()


def solution(mesh):
    sizes = {a: mesh.shape[a] for a in ("gx", "gy", "gz")}

    def per_device(density, momentum, hydrogen, forced_modes):
        local = density.shape
        size_x, size_y, size_z = local
        rows = size_x * size_y
        full = (size_x * sizes["gx"], size_y * sizes["gy"], size_z * sizes["gz"])
        early, back, late = tables(local, full)
        modes = forced_modes.T
        stages = plan(sizes)
        messages = sum(len(g) for g in stages)
        any_spec = pl.BlockSpec(memory_space=pl.ANY)
        f32 = jnp.float32
        rates = pl.pallas_call(
            functools.partial(kernel, sizes, local),
            out_shape=[pltpu.VMEM(local, f32)] * 3,
            in_specs=[any_spec] * 7,
            out_specs=[pl.BlockSpec(memory_space=pltpu.VMEM)] * 3,
            scratch_shapes=[
                pltpu.VMEM((3, size_x + 2 * REACH, size_y, size_z), f32),
                pltpu.VMEM(modes.shape, jnp.int32),
                pltpu.VMEM(early.shape, jnp.bfloat16),
                pltpu.VMEM(back.shape, jnp.bfloat16),
                pltpu.VMEM(late.shape, f32),
                pltpu.VMEM((2, size_x, size_y + 16, size_z), f32),
                pltpu.VMEM((2, 2, size_x, 8, size_z), f32),
                pltpu.VMEM((2, size_x, 8, size_z), f32),
                pltpu.VMEM((2, 8, rows), f32),
                pltpu.VMEM((2, 2, 8, rows), f32),
                pltpu.VMEM((len(stages), ROWS, 2 * HALF), f32),
                pltpu.VMEM((messages, ROWS, 2 * HALF), f32),
                pltpu.SemaphoreType.DMA((7,)),
                pltpu.SemaphoreType.DMA((6,)),
                pltpu.SemaphoreType.DMA((6,)),
                pltpu.SemaphoreType.DMA((len(stages),)),
                pltpu.SemaphoreType.DMA((len(stages),)),
            ],
            compiler_params=pltpu.CompilerParams(collective_id=0, has_side_effects=True),
            name="flame",
        )(density, momentum, hydrogen, modes, jnp.asarray(early), jnp.asarray(back), jnp.asarray(late))
        return tuple(pl.pallas_call(
            write_out,
            out_shape=[jax.ShapeDtypeStruct(local, f32)] * 3,
            in_specs=[pl.BlockSpec(memory_space=pltpu.VMEM)] * 3,
            out_specs=[any_spec] * 3,
            scratch_shapes=[pltpu.SemaphoreType.DMA((3,))],
            name="write",
        )(*[pltpu.with_memory_space_constraint(r, pltpu.VMEM) for r in rates]))

    in_specs = (P("gx", "gy", "gz"), P("gx", "gy", "gz"), P("gx", "gy", "gz"), P())
    out_specs = (P("gx", "gy", "gz"), P("gx", "gy", "gz"), P("gx", "gy", "gz"))
    return jax.shard_map(
        per_device, mesh=mesh, in_specs=in_specs, out_specs=out_specs, check_vma=False
    )
```

```python
import functools
import math

import jax
import jax.numpy as jnp
import numpy as np
from jax import lax
from jax.experimental import pallas as pl
from jax.experimental.pallas import tpu as pltpu
from jax.sharding import PartitionSpec as P

KMAX = 3
WIDTH = 2 * KMAX + 1
HALF = 64
ROWS = KMAX + 1
REACH = 4

FIRST_COEFFS = (0.8, -0.2, 4.0 / 105.0, -1.0 / 280.0)
SECOND_COEFFS = (1.6, -0.2, 8.0 / 315.0, -1.0 / 560.0)
CENTRE_COEFF = -205.0 / 72.0
VISCOSITY = 0.3
DIFFUSIVITY = 1.5
FORCE_POWER = 0.3
ENERGY_EPS = 1e-06
ACTIVATION = 2.0
HIGHEST = lax.Precision.HIGHEST
MESH = pl.DeviceIdType.MESH


def packed_modes():
    reach = range(-KMAX, KMAX + 1)
    cells = [(x, y, z) for z in range(ROWS) for x in reach for y in reach
             if x * x + y * y + z * z <= KMAX * KMAX and (z, x, y) > (0, 0, 0)]
    return cells


def packed_index(place):
    cells = packed_modes()
    result = []
    for part in range(3):
        value = jnp.full(place.shape, cells[0][part], jnp.int32)
        if part == 1:
            value = value + place
        for i in range(1, len(cells)):
            step = cells[i][part] - cells[i - 1][part] - (part == 1)
            if step:
                value = value + jnp.where(place >= i, step, 0)
        result.append(value)
    return result


def tables(local, full):
    size_x, size_y, size_z = local
    full_x, full_y, full_z = full
    k = np.arange(-KMAX, KMAX + 1)
    ang_z = 2.0 * np.pi * (k[:, None] * np.arange(size_z)[None, :]) / full_z
    trig_z = np.zeros((2 * ROWS, size_z))
    trig_z[:ROWS] = np.cos(ang_z[KMAX:])
    trig_z[ROWS:] = np.sin(ang_z[KMAX:])
    ax = k[:, None] * np.arange(size_x)[None, :] / full_x
    ay = k[:, None] * np.arange(size_y)[None, :] / full_y
    ang = np.stack([2.0 * np.pi * (ax[x + KMAX, :, None] + ay[y + KMAX, None, :]) for x, y, _ in packed_modes()])
    ang = ang.reshape(-1, size_x * size_y)
    trig_xy = np.zeros((2 * HALF, size_x * size_y))
    trig_xy[: len(ang)] = np.cos(ang)
    trig_xy[HALF : HALF + len(ang)] = np.sin(ang)
    edge = np.zeros((8, size_z))
    for j in range(REACH):
        edge[j, j] = 1.0
        edge[REACH + j, size_z - REACH + j] = 1.0
    band = np.zeros((size_z, size_z))
    halo = np.zeros((16, size_z))
    for z in range(size_z):
        band[z, z] = 3.0 * CENTRE_COEFF
        for offset, weight in enumerate(SECOND_COEFFS, 1):
            for q in (z - offset, z + offset):
                if 0 <= q < size_z:
                    band[q, z] = weight
                elif q < 0:
                    halo[8 + q, z] = weight
                else:
                    halo[8 + q - size_z, z] = weight
    z_high, z_low = split_host(trig_z)
    xy_high, xy_low = split_host(trig_xy)
    early = np.concatenate([z_high, z_low, xy_high, xy_low, z_high, z_high, z_low, z_low,
                            split_host(np.concatenate([edge, np.zeros_like(edge)], 0))[0]], 0)
    back = np.concatenate([xy_high, xy_low], 1)
    late = np.concatenate([halo, band], 0).astype(np.float32)
    return early, back, late


def split_host(table):
    high = table.astype(np.float32).astype(jnp.bfloat16)
    low = (table - high.astype(np.float64)).astype(np.float32).astype(jnp.bfloat16)
    return high, low


def split(x):
    high = x.astype(jnp.bfloat16).astype(jnp.float32)
    return high, x - high


def dot_split(a, b, contract):
    return lax.dot_general(a.astype(jnp.bfloat16), b.astype(jnp.bfloat16), (contract, ((), ())),
                           preferred_element_type=jnp.float32)


def fold(x):
    rows, lanes = x.shape
    x = x[: rows // 2] + x[rows // 2 :]
    return x[:, : lanes // 2] + x[:, lanes // 2 :]


def dot_nt(a, b):
    return lax.dot_general(a, b, (((1,), (1,)), ((), ())), precision=HIGHEST, preferred_element_type=jnp.float32)


def dot_nn(a, b):
    return lax.dot_general(a, b, (((1,), (0,)), ((), ())), precision=HIGHEST, preferred_element_type=jnp.float32)


def dot_tn(a, b):
    return lax.dot_general(a, b, (((0,), (0,)), ((), ())), precision=HIGHEST, preferred_element_type=jnp.float32)


def group_offsets(sizes, axes):
    offsets = [{}]
    for axis in axes:
        offsets = [{**o, axis: s} for o in offsets for s in range(sizes[axis])]
    return [o for o in offsets if any(o.values())]


def tree_sum(parts):
    parts = list(parts)
    while len(parts) > 1:
        parts = [sum(parts[i : i + 2][1:], parts[i]) for i in range(0, len(parts), 2)]
    return parts[0]


def plan(sizes):
    if math.prod(sizes.values()) <= 32:
        stages = [("gz", "gy", "gx")]
    elif sizes["gx"] * sizes["gy"] <= 16:
        stages = [("gz",), ("gx", "gy")]
    else:
        stages = [("gz",), ("gx",), ("gy",)]
    return [group_offsets(sizes, s)[::-1] for s in stages]


def kernel(sizes, local, dens_hbm, mom_hbm, fuel_hbm, modes_hbm, early_hbm, back_hbm, late_hbm,
           drate, mrate, hrate,
           f, modes, early, back, late, edges, sides, ypack, zpack, ztile, stage_own, stage_got,
           load_sem, halo_send, halo_recv, stage_send, stage_recv):
    size_x, size_y, size_z = local
    rows = size_x * size_y
    rows_z = 2 * ROWS
    me = {a: lax.axis_index(a) for a in sizes}
    stages = plan(sizes)

    def at(offset):
        return {a: lax.rem(me[a] + o, sizes[a]) for a, o in offset.items()}

    own = pl.ds(REACH, size_x)
    loads = [
        pltpu.make_async_copy(src, dst, load_sem.at[i])
        for i, (src, dst) in enumerate([
            (dens_hbm, f.at[0, own]), (mom_hbm, f.at[1, own]), (early_hbm, early),
            (fuel_hbm, f.at[2, own]), (modes_hbm, modes), (late_hbm, late), (back_hbm, back),
        ])
    ]
    for copy in loads:
        copy.start()
    barrier = pltpu.get_barrier_semaphore()
    partners = [o for group in stages for o in group]
    for offset in partners:
        pl.semaphore_signal(barrier, inc=1, device_id=at(offset), device_id_type=MESH)

    lane = lax.broadcasted_iota(jnp.int32, (1, 2 * HALF), 1)
    kx, ky, kz = packed_index(lax.rem(lane, HALF))
    turn = jnp.zeros((1, 2 * HALF), jnp.float32)
    for k, axis in ((kx, "gx"), (ky, "gy"), (kz, "gz")):
        part = k.astype(jnp.float32) * me[axis].astype(jnp.float32) / sizes[axis]
        turn = turn + (part - jnp.floor(part))
    level = (lax.broadcasted_iota(jnp.int32, (ROWS, 2 * HALF), 0) == kz).astype(jnp.float32)
    turn = turn - jnp.floor(turn + 0.5)
    cos_p = jnp.cos(2.0 * math.pi * turn)
    sin_p = jnp.sin(2.0 * math.pi * turn)
    sign = jnp.where(lane < HALF, -1.0, 1.0)
    sin_p = sign * sin_p

    loads[0].wait()
    loads[1].wait()
    loads[2].wait()
    flat = lambda i: f[i, own].reshape(rows, size_z)
    vel = flat(1) / flat(0)
    deep = 2 * rows_z
    table_xy = early[deep : deep + 4 * HALF]
    vel_both = jnp.concatenate(split(vel), 0)
    part = fold(dot_split(early[0:deep], vel_both, ((1,), (1,))))
    grid = fold(dot_split(jnp.concatenate(split(part), 0), table_xy, ((1,), (1,))))
    grid = grid * jnp.concatenate([level, level], 0)
    flip = jnp.sum(grid[ROWS:], axis=0, keepdims=True)
    cube = jnp.sum(grid[0:ROWS], axis=0, keepdims=True) + sign * pltpu.roll(flip, HALF, 1)
    cube = cos_p * cube + sin_p * pltpu.roll(cube, HALF, 1)
    stage_own[0] = cube

    def span(s):
        base = sum(len(g) for g in stages[:s])
        return pl.ds(base, len(stages[s]))

    def send_stage(s):
        base = sum(len(g) for g in stages[:s])
        for i, offset in enumerate(stages[s]):
            pltpu.make_async_remote_copy(
                src_ref=stage_own.at[s], dst_ref=stage_got.at[base + i],
                send_sem=stage_send.at[s], recv_sem=stage_recv.at[s],
                device_id=at(offset), device_id_type=MESH).start()

    def wait_stage(s, sem):
        got = stage_got.at[span(s)]
        pltpu.make_async_copy(got, got, sem.at[s]).wait()

    def sum_stage(s):
        base = sum(len(g) for g in stages[:s])
        wait_stage(s, stage_recv)
        return tree_sum([stage_own[s]] + [stage_got[base + i] for i in range(len(stages[s]))])

    loads[3].wait()
    pieces = []
    for i in range(2):
        ypack[i, :, 0:REACH] = f[1 + i, own, 0:REACH]
        ypack[i, :, REACH : 2 * REACH] = f[1 + i, own, size_y - REACH : size_y]
        high, rest = split(flat(1 + i))
        pieces += [high, *split(rest)]
    edge_at = deep + 4 * HALF + 4 * rows_z
    ends = dot_split(early[edge_at : edge_at + 16], jnp.concatenate(pieces, 0), ((1,), (1,)))[0:8]
    for i in range(2):
        zpack[i] = tree_sum([ends[:, (3 * i + j) * rows : (3 * i + j + 1) * rows] for j in range(3)])

    pl.semaphore_wait(barrier, len(partners))
    send_stage(0)

    def send(src, dst, slot, axis, step):
        copy = pltpu.make_async_remote_copy(
            src_ref=src, dst_ref=dst, send_sem=halo_send.at[slot], recv_sem=halo_recv.at[slot],
            device_id=at({axis: step % sizes[axis]}), device_id_type=MESH)
        copy.start()
        return copy

    halos_x = [
        send(f.at[:, pl.ds(size_x, REACH)], f.at[:, pl.ds(0, REACH)], 0, "gx", 1),
        send(f.at[:, pl.ds(REACH, REACH)], f.at[:, pl.ds(size_x + REACH, REACH)], 1, "gx", -1),
    ]
    halos_y = [send(ypack, sides.at[0], 2, "gy", 1)]
    if sizes["gy"] > 2:
        halos_y.append(send(ypack, sides.at[1], 3, "gy", -1))
    halos_z = [send(zpack, ztile.at[0], 4, "gz", 1), send(zpack, ztile.at[1], 5, "gz", -1)]

    loads[4].wait()
    count = modes.shape[1]
    code = (modes[0:1] * WIDTH + modes[1:2]) * WIDTH + modes[2:3]
    place = lax.rem(lax.broadcasted_iota(jnp.int32, (2 * HALF, 1), 0), HALF)
    px, py, pz = packed_index(place)
    mine = (px * WIDTH + py) * WIDTH + pz
    used = place < len(packed_modes())
    both_ways = jnp.where(used & (mine == code), 1.0, 0.0) + jnp.where(used & (mine == -code), 1.0, 0.0)
    chosen = dot_nt(jnp.ones((8, count), jnp.float32), both_ways)[0:1]

    loads[5].wait()
    lap = [dot_nn(flat(1 + i), late[16 : 16 + size_z]).reshape(size_x, size_y, size_z) for i in range(2)]
    outs = (drate, mrate, hrate)
    mrate[...] = lap[0]
    hrate[...] = lap[1]

    for s in range(1, len(stages)):
        stage_own[s] = sum_stage(s - 1)
        send_stage(s)

    for copy in halos_z:
        copy.wait_recv()
    for copy in halos_y:
        copy.wait_recv()
    for i in range(2):
        tile = jnp.concatenate([ztile[0, i], ztile[1, i]], 0)
        edges[i, :, 0:8] = sides[0, i]
        edges[i, :, 8 : 8 + size_y] = f[1 + i, own]
        edges[i, :, 8 + size_y : 16 + size_y] = sides[1 if sizes["gy"] > 2 else 0, i]
        total = outs[1 + i][...] + dot_tn(tile, late[0:16]).reshape(size_x, size_y, size_z)
        for offset, weight in enumerate(SECOND_COEFFS, 1):
            total = total + weight * (
                edges[i, :, 8 + offset : 8 + offset + size_y] + edges[i, :, 8 - offset : 8 - offset + size_y])
        outs[1 + i][...] = total

    for copy in halos_x:
        copy.wait_recv()
    def planes(x, offset):
        return x[REACH + offset : REACH + offset + size_x]

    def first_diff(x):
        total = None
        for offset, weight in enumerate(FIRST_COEFFS, 1):
            term = weight * (planes(x, offset) - planes(x, -offset))
            total = term if total is None else total + term
        return total

    def second_diff(x):
        return tree_sum([w * (planes(x, o) + planes(x, -o)) for o, w in enumerate(SECOND_COEFFS, 1)])

    mom = f[1]
    dens = f[0]
    fuel = f[2]
    vel_pad = mom / dens
    drate[...] = -first_diff(mom)
    mid_fuel = planes(fuel, 0)
    hrate[...] = (DIFFUSIVITY * (hrate[...] + second_diff(fuel)) - first_diff(fuel * vel_pad)
                  - mid_fuel * jnp.exp(-ACTIVATION * mid_fuel / planes(dens, 0)))
    mrate[...] = VISCOSITY * (mrate[...] + second_diff(mom)) - first_diff(mom * vel_pad + dens)

    loads[6].wait()
    ncell = float(rows * size_z * math.prod(sizes.values()))
    cube = sum_stage(len(stages) - 1)
    coef = cube / ncell
    picked = chosen * coef
    energy = jnp.sum(jnp.sum(picked * coef, axis=1, keepdims=True), axis=0, keepdims=True)
    scale = 2.0 * FORCE_POWER / (energy + ENERGY_EPS)
    local_coef = cos_p * picked - sin_p * pltpu.roll(picked, HALF, 1)
    both = jnp.concatenate([level * local_coef, level * (-sign * pltpu.roll(local_coef, HALF, 1))], 0)
    wave = fold(dot_split(jnp.concatenate(split(both), 0), back[...], ((1,), (0,))))
    high, rest = split(wave)
    waves = jnp.concatenate([high, rest, high, rest], 0).T
    low = dot_split(waves, early[deep + 4 * HALF : deep + 4 * HALF + 4 * rows_z], ((1,), (0,)))
    low = low.reshape(size_x, size_y, size_z)
    mrate[...] = mrate[...] + f[0, own] * (low * scale.reshape(1, 1, 1))
    for copy in halos_x + halos_y + halos_z:
        copy.wait_send()
    for s in range(len(stages)):
        wait_stage(s, stage_send)


def write_out(*refs):
    count = len(refs) // 2
    copies = [pltpu.make_async_copy(refs[i], refs[count + i], refs[-1].at[i]) for i in range(count)]
    for copy in copies:
        copy.start()
    for copy in copies:
        copy.wait()


def solution(mesh):
    sizes = {a: mesh.shape[a] for a in ("gx", "gy", "gz")}

    def per_device(density, momentum, hydrogen, forced_modes):
        local = density.shape
        size_x, size_y, size_z = local
        rows = size_x * size_y
        full = (size_x * sizes["gx"], size_y * sizes["gy"], size_z * sizes["gz"])
        early, back, late = tables(local, full)
        modes = forced_modes.T
        stages = plan(sizes)
        messages = sum(len(g) for g in stages)
        any_spec = pl.BlockSpec(memory_space=pl.ANY)
        f32 = jnp.float32
        rates = pl.pallas_call(
            functools.partial(kernel, sizes, local),
            out_shape=[pltpu.VMEM(local, f32)] * 3,
            in_specs=[any_spec] * 7,
            out_specs=[pl.BlockSpec(memory_space=pltpu.VMEM)] * 3,
            scratch_shapes=[
                pltpu.VMEM((3, size_x + 2 * REACH, size_y, size_z), f32),
                pltpu.VMEM(modes.shape, jnp.int32),
                pltpu.VMEM(early.shape, jnp.bfloat16),
                pltpu.VMEM(back.shape, jnp.bfloat16),
                pltpu.VMEM(late.shape, f32),
                pltpu.VMEM((2, size_x, size_y + 16, size_z), f32),
                pltpu.VMEM((2, 2, size_x, 8, size_z), f32),
                pltpu.VMEM((2, size_x, 8, size_z), f32),
                pltpu.VMEM((2, 8, rows), f32),
                pltpu.VMEM((2, 2, 8, rows), f32),
                pltpu.VMEM((len(stages), 1, 2 * HALF), f32),
                pltpu.VMEM((messages, 1, 2 * HALF), f32),
                pltpu.SemaphoreType.DMA((7,)),
                pltpu.SemaphoreType.DMA((6,)),
                pltpu.SemaphoreType.DMA((6,)),
                pltpu.SemaphoreType.DMA((len(stages),)),
                pltpu.SemaphoreType.DMA((len(stages),)),
            ],
            compiler_params=pltpu.CompilerParams(collective_id=0, has_side_effects=True),
            name="flame",
        )(density, momentum, hydrogen, modes, jnp.asarray(early), jnp.asarray(back), jnp.asarray(late))
        return tuple(pl.pallas_call(
            write_out,
            out_shape=[jax.ShapeDtypeStruct(local, f32)] * 3,
            in_specs=[pl.BlockSpec(memory_space=pltpu.VMEM)] * 3,
            out_specs=[any_spec] * 3,
            scratch_shapes=[pltpu.SemaphoreType.DMA((3,))],
            name="write",
        )(*[pltpu.with_memory_space_constraint(r, pltpu.VMEM) for r in rates]))

    in_specs = (P("gx", "gy", "gz"), P("gx", "gy", "gz"), P("gx", "gy", "gz"), P())
    out_specs = (P("gx", "gy", "gz"), P("gx", "gy", "gz"), P("gx", "gy", "gz"))
    return jax.shard_map(
        per_device, mesh=mesh, in_specs=in_specs, out_specs=out_specs, check_vma=False
    )
```

```python
import functools
import math

import jax
import jax.numpy as jnp
import numpy as np
from jax import lax
from jax.experimental import pallas as pl
from jax.experimental.pallas import tpu as pltpu
from jax.sharding import PartitionSpec as P

KMAX = 3
WIDTH = 2 * KMAX + 1
HALF = 64
ROWS = KMAX + 1
REACH = 4

FIRST_COEFFS = (0.8, -0.2, 4.0 / 105.0, -1.0 / 280.0)
SECOND_COEFFS = (1.6, -0.2, 8.0 / 315.0, -1.0 / 560.0)
CENTRE_COEFF = -205.0 / 72.0
VISCOSITY = 0.3
DIFFUSIVITY = 1.5
FORCE_POWER = 0.3
ENERGY_EPS = 1e-06
ACTIVATION = 2.0
HIGHEST = lax.Precision.HIGHEST
MESH = pl.DeviceIdType.MESH


def packed_modes():
    reach = range(-KMAX, KMAX + 1)
    cells = [(x, y, z) for z in range(ROWS) for x in reach for y in reach
             if x * x + y * y + z * z <= KMAX * KMAX and (z, x, y) > (0, 0, 0)]
    return cells


def packed_index(place):
    cells = packed_modes()
    result = []
    for part in range(3):
        value = jnp.full(place.shape, cells[0][part], jnp.int32)
        if part == 1:
            value = value + place
        for i in range(1, len(cells)):
            step = cells[i][part] - cells[i - 1][part] - (part == 1)
            if step:
                value = value + jnp.where(place >= i, step, 0)
        result.append(value)
    return result


def tables(local, full):
    size_x, size_y, size_z = local
    full_x, full_y, full_z = full
    k = np.arange(-KMAX, KMAX + 1)
    ang_z = 2.0 * np.pi * (k[:, None] * np.arange(size_z)[None, :]) / full_z
    trig_z = np.zeros((2 * ROWS, size_z))
    trig_z[:ROWS] = np.cos(ang_z[KMAX:])
    trig_z[ROWS:] = np.sin(ang_z[KMAX:])
    ax = k[:, None] * np.arange(size_x)[None, :] / full_x
    ay = k[:, None] * np.arange(size_y)[None, :] / full_y
    ang = np.stack([2.0 * np.pi * (ax[x + KMAX, :, None] + ay[y + KMAX, None, :]) for x, y, _ in packed_modes()])
    ang = ang.reshape(-1, size_x * size_y)
    trig_xy = np.zeros((2 * HALF, size_x * size_y))
    trig_xy[: len(ang)] = np.cos(ang)
    trig_xy[HALF : HALF + len(ang)] = np.sin(ang)
    edge = np.zeros((8, size_z))
    for j in range(REACH):
        edge[j, j] = 1.0
        edge[REACH + j, size_z - REACH + j] = 1.0
    band = np.zeros((size_z, size_z))
    halo = np.zeros((16, size_z))
    for z in range(size_z):
        band[z, z] = 3.0 * CENTRE_COEFF
        for offset, weight in enumerate(SECOND_COEFFS, 1):
            for q in (z - offset, z + offset):
                if 0 <= q < size_z:
                    band[q, z] = weight
                elif q < 0:
                    halo[8 + q, z] = weight
                else:
                    halo[8 + q - size_z, z] = weight
    z_high, z_low = split_host(trig_z)
    xy_high, xy_low = split_host(trig_xy)
    early = np.concatenate([z_high, z_low, xy_high, xy_low, z_high, z_high, z_low, z_low,
                            split_host(np.concatenate([edge, np.zeros_like(edge)], 0))[0]], 0)
    back = np.concatenate([xy_high, xy_low], 1)
    late = np.concatenate([halo, band], 0).astype(np.float32)
    return early, back, late


def split_host(table):
    high = table.astype(np.float32).astype(jnp.bfloat16)
    low = (table - high.astype(np.float64)).astype(np.float32).astype(jnp.bfloat16)
    return high, low


def split(x):
    high = x.astype(jnp.bfloat16).astype(jnp.float32)
    return high, x - high


def dot_split(a, b, contract):
    return lax.dot_general(a.astype(jnp.bfloat16), b.astype(jnp.bfloat16), (contract, ((), ())),
                           preferred_element_type=jnp.float32)


def fold(x):
    rows, lanes = x.shape
    x = x[: rows // 2] + x[rows // 2 :]
    return x[:, : lanes // 2] + x[:, lanes // 2 :]


def dot_nt(a, b):
    return lax.dot_general(a, b, (((1,), (1,)), ((), ())), precision=HIGHEST, preferred_element_type=jnp.float32)


def dot_nn(a, b):
    return lax.dot_general(a, b, (((1,), (0,)), ((), ())), precision=HIGHEST, preferred_element_type=jnp.float32)


def dot_tn(a, b):
    return lax.dot_general(a, b, (((0,), (0,)), ((), ())), precision=HIGHEST, preferred_element_type=jnp.float32)


def group_offsets(sizes, axes):
    offsets = [{}]
    for axis in axes:
        offsets = [{**o, axis: s} for o in offsets for s in range(sizes[axis])]
    return [o for o in offsets if any(o.values())]


def tree_sum(parts):
    parts = list(parts)
    while len(parts) > 1:
        parts = [sum(parts[i : i + 2][1:], parts[i]) for i in range(0, len(parts), 2)]
    return parts[0]


def plan(sizes):
    if math.prod(sizes.values()) <= 32:
        stages = [("gz", "gy", "gx")]
    elif sizes["gx"] * sizes["gy"] <= 16:
        stages = [("gz",), ("gx", "gy")]
    else:
        stages = [("gz",), ("gx",), ("gy",)]
    return [group_offsets(sizes, s)[::-1] for s in stages]


def kernel(sizes, local, dens_hbm, mom_hbm, fuel_hbm, modes_hbm, early_hbm, back_hbm, late_hbm,
           drate, mrate, hrate,
           f, modes, early, back, late, edges, sides, ypack, zpack, ztile, stage_own, stage_got,
           load_sem, halo_send, halo_recv, stage_send, stage_recv):
    size_x, size_y, size_z = local
    rows = size_x * size_y
    rows_z = 2 * ROWS
    me = {a: lax.axis_index(a) for a in sizes}
    stages = plan(sizes)

    def at(offset):
        return {a: lax.rem(me[a] + o, sizes[a]) for a, o in offset.items()}

    own = pl.ds(REACH, size_x)
    loads = [
        pltpu.make_async_copy(src, dst, load_sem.at[i])
        for i, (src, dst) in enumerate([
            (dens_hbm, f.at[0, own]), (mom_hbm, f.at[1, own]), (early_hbm, early),
            (fuel_hbm, f.at[2, own]), (modes_hbm, modes), (late_hbm, late), (back_hbm, back),
        ])
    ]
    for copy in loads:
        copy.start()
    barrier = pltpu.get_barrier_semaphore()
    partners = [o for group in stages for o in group]
    for offset in partners:
        pl.semaphore_signal(barrier, inc=1, device_id=at(offset), device_id_type=MESH)

    lane = lax.broadcasted_iota(jnp.int32, (1, 2 * HALF), 1)
    kx, ky, kz = packed_index(lax.rem(lane, HALF))
    turn = jnp.zeros((1, 2 * HALF), jnp.float32)
    for k, axis in ((kx, "gx"), (ky, "gy"), (kz, "gz")):
        part = k.astype(jnp.float32) * me[axis].astype(jnp.float32) / sizes[axis]
        turn = turn + (part - jnp.floor(part))
    level = (lax.broadcasted_iota(jnp.int32, (ROWS, 2 * HALF), 0) == kz).astype(jnp.float32)
    turn = turn - jnp.floor(turn + 0.5)
    cos_p = jnp.cos(2.0 * math.pi * turn)
    sin_p = jnp.sin(2.0 * math.pi * turn)
    sign = jnp.where(lane < HALF, -1.0, 1.0)
    sin_p = sign * sin_p

    loads[0].wait()
    loads[1].wait()
    loads[2].wait()
    flat = lambda i: f[i, own].reshape(rows, size_z)
    vel = flat(1) / flat(0)
    deep = 2 * rows_z
    table_xy = early[deep : deep + 4 * HALF]
    vel_both = jnp.concatenate(split(vel), 0)
    part = fold(dot_split(early[0:deep], vel_both, ((1,), (1,))))
    grid = fold(dot_split(jnp.concatenate(split(part), 0), table_xy, ((1,), (1,))))
    grid = grid * jnp.concatenate([level, level], 0)
    flip = jnp.sum(grid[ROWS:], axis=0, keepdims=True)
    cube = jnp.sum(grid[0:ROWS], axis=0, keepdims=True) + sign * pltpu.roll(flip, HALF, 1)
    cube = cos_p * cube + sin_p * pltpu.roll(cube, HALF, 1)
    stage_own[0] = cube

    def span(s):
        base = sum(len(g) for g in stages[:s])
        return pl.ds(base, len(stages[s]))

    def send_stage(s):
        base = sum(len(g) for g in stages[:s])
        for i, offset in enumerate(stages[s]):
            pltpu.make_async_remote_copy(
                src_ref=stage_own.at[s], dst_ref=stage_got.at[base + i],
                send_sem=stage_send.at[s], recv_sem=stage_recv.at[s],
                device_id=at(offset), device_id_type=MESH).start()

    def wait_stage(s, sem):
        got = stage_got.at[span(s)]
        pltpu.make_async_copy(got, got, sem.at[s]).wait()

    def sum_stage(s):
        base = sum(len(g) for g in stages[:s])
        wait_stage(s, stage_recv)
        return tree_sum([stage_own[s]] + [stage_got[base + i] for i in range(len(stages[s]))])

    loads[3].wait()
    pieces = []
    for i in range(2):
        ypack[i, :, 0:REACH] = f[1 + i, own, 0:REACH]
        ypack[i, :, REACH : 2 * REACH] = f[1 + i, own, size_y - REACH : size_y]
        high, rest = split(flat(1 + i))
        pieces += [high, *split(rest)]
    edge_at = deep + 4 * HALF + 4 * rows_z
    ends = dot_split(early[edge_at : edge_at + 16], jnp.concatenate(pieces, 0), ((1,), (1,)))[0:8]
    for i in range(2):
        zpack[i] = tree_sum([ends[:, (3 * i + j) * rows : (3 * i + j + 1) * rows] for j in range(3)])

    pl.semaphore_wait(barrier, len(partners))
    send_stage(0)

    def send(src, dst, slot, axis, step):
        copy = pltpu.make_async_remote_copy(
            src_ref=src, dst_ref=dst, send_sem=halo_send.at[slot // 2], recv_sem=halo_recv.at[slot // 2],
            device_id=at({axis: step % sizes[axis]}), device_id_type=MESH)
        copy.start()
        return copy

    halos_x = [
        send(f.at[:, pl.ds(size_x, REACH)], f.at[:, pl.ds(0, REACH)], 0, "gx", 1),
        send(f.at[:, pl.ds(REACH, REACH)], f.at[:, pl.ds(size_x + REACH, REACH)], 1, "gx", -1),
    ]
    halos_y = [send(ypack, sides.at[0], 2, "gy", 1)]
    if sizes["gy"] > 2:
        halos_y.append(send(ypack, sides.at[1], 3, "gy", -1))
    halos_z = [send(zpack, ztile.at[0], 4, "gz", 1), send(zpack, ztile.at[1], 5, "gz", -1)]

    loads[4].wait()
    count = modes.shape[1]
    code = (modes[0:1] * WIDTH + modes[1:2]) * WIDTH + modes[2:3]
    place = lax.rem(lax.broadcasted_iota(jnp.int32, (2 * HALF, 1), 0), HALF)
    px, py, pz = packed_index(place)
    mine = (px * WIDTH + py) * WIDTH + pz
    used = place < len(packed_modes())
    both_ways = jnp.where(used & (mine == code), 1.0, 0.0) + jnp.where(used & (mine == -code), 1.0, 0.0)
    chosen = dot_nt(jnp.ones((8, count), jnp.float32), both_ways)[0:1]

    loads[5].wait()
    lap = [dot_nn(flat(1 + i), late[16 : 16 + size_z]).reshape(size_x, size_y, size_z) for i in range(2)]
    outs = (drate, mrate, hrate)
    mrate[...] = lap[0]
    hrate[...] = lap[1]

    for s in range(1, len(stages)):
        stage_own[s] = sum_stage(s - 1)
        send_stage(s)

    arrived = [f.at[:, pl.ds(0, 2 * REACH)], sides.at[pl.ds(0, len(halos_y))], ztile]
    def wait_halo(sem, slot):
        pltpu.make_async_copy(arrived[slot], arrived[slot], sem.at[slot]).wait()

    wait_halo(halo_recv, 2)
    wait_halo(halo_recv, 1)
    for i in range(2):
        tile = jnp.concatenate([ztile[0, i], ztile[1, i]], 0)
        edges[i, :, 0:8] = sides[0, i]
        edges[i, :, 8 : 8 + size_y] = f[1 + i, own]
        edges[i, :, 8 + size_y : 16 + size_y] = sides[1 if sizes["gy"] > 2 else 0, i]
        total = outs[1 + i][...] + dot_tn(tile, late[0:16]).reshape(size_x, size_y, size_z)
        for offset, weight in enumerate(SECOND_COEFFS, 1):
            total = total + weight * (
                edges[i, :, 8 + offset : 8 + offset + size_y] + edges[i, :, 8 - offset : 8 - offset + size_y])
        outs[1 + i][...] = total

    wait_halo(halo_recv, 0)
    def planes(x, offset):
        return x[REACH + offset : REACH + offset + size_x]

    def first_diff(x):
        total = None
        for offset, weight in enumerate(FIRST_COEFFS, 1):
            term = weight * (planes(x, offset) - planes(x, -offset))
            total = term if total is None else total + term
        return total

    def second_diff(x):
        return tree_sum([w * (planes(x, o) + planes(x, -o)) for o, w in enumerate(SECOND_COEFFS, 1)])

    mom = f[1]
    dens = f[0]
    fuel = f[2]
    vel_pad = mom / dens
    drate[...] = -first_diff(mom)
    mid_fuel = planes(fuel, 0)
    hrate[...] = (DIFFUSIVITY * (hrate[...] + second_diff(fuel)) - first_diff(fuel * vel_pad)
                  - mid_fuel * jnp.exp(-ACTIVATION * mid_fuel / planes(dens, 0)))
    mrate[...] = VISCOSITY * (mrate[...] + second_diff(mom)) - first_diff(mom * vel_pad + dens)

    loads[6].wait()
    ncell = float(rows * size_z * math.prod(sizes.values()))
    cube = sum_stage(len(stages) - 1)
    coef = cube / ncell
    picked = chosen * coef
    energy = jnp.sum(jnp.sum(picked * coef, axis=1, keepdims=True), axis=0, keepdims=True)
    scale = 2.0 * FORCE_POWER / (energy + ENERGY_EPS)
    local_coef = cos_p * picked - sin_p * pltpu.roll(picked, HALF, 1)
    both = jnp.concatenate([level * local_coef, level * (-sign * pltpu.roll(local_coef, HALF, 1))], 0)
    wave = fold(dot_split(jnp.concatenate(split(both), 0), back[...], ((1,), (0,))))
    high, rest = split(wave)
    waves = jnp.concatenate([high, rest, high, rest], 0).T
    low = dot_split(waves, early[deep + 4 * HALF : deep + 4 * HALF + 4 * rows_z], ((1,), (0,)))
    low = low.reshape(size_x, size_y, size_z)
    mrate[...] = mrate[...] + f[0, own] * (low * scale.reshape(1, 1, 1))
    for slot in range(3):
        wait_halo(halo_send, slot)
    for s in range(len(stages)):
        wait_stage(s, stage_send)


def write_out(*refs):
    count = len(refs) // 2
    copies = [pltpu.make_async_copy(refs[i], refs[count + i], refs[-1].at[i]) for i in range(count)]
    for copy in copies:
        copy.start()
    for copy in copies:
        copy.wait()


def solution(mesh):
    sizes = {a: mesh.shape[a] for a in ("gx", "gy", "gz")}

    def per_device(density, momentum, hydrogen, forced_modes):
        local = density.shape
        size_x, size_y, size_z = local
        rows = size_x * size_y
        full = (size_x * sizes["gx"], size_y * sizes["gy"], size_z * sizes["gz"])
        early, back, late = tables(local, full)
        modes = forced_modes.T
        stages = plan(sizes)
        messages = sum(len(g) for g in stages)
        any_spec = pl.BlockSpec(memory_space=pl.ANY)
        f32 = jnp.float32
        rates = pl.pallas_call(
            functools.partial(kernel, sizes, local),
            out_shape=[pltpu.VMEM(local, f32)] * 3,
            in_specs=[any_spec] * 7,
            out_specs=[pl.BlockSpec(memory_space=pltpu.VMEM)] * 3,
            scratch_shapes=[
                pltpu.VMEM((3, size_x + 2 * REACH, size_y, size_z), f32),
                pltpu.VMEM(modes.shape, jnp.int32),
                pltpu.VMEM(early.shape, jnp.bfloat16),
                pltpu.VMEM(back.shape, jnp.bfloat16),
                pltpu.VMEM(late.shape, f32),
                pltpu.VMEM((2, size_x, size_y + 16, size_z), f32),
                pltpu.VMEM((2, 2, size_x, 8, size_z), f32),
                pltpu.VMEM((2, size_x, 8, size_z), f32),
                pltpu.VMEM((2, 8, rows), f32),
                pltpu.VMEM((2, 2, 8, rows), f32),
                pltpu.VMEM((len(stages), 1, 2 * HALF), f32),
                pltpu.VMEM((messages, 1, 2 * HALF), f32),
                pltpu.SemaphoreType.DMA((7,)),
                pltpu.SemaphoreType.DMA((3,)),
                pltpu.SemaphoreType.DMA((3,)),
                pltpu.SemaphoreType.DMA((len(stages),)),
                pltpu.SemaphoreType.DMA((len(stages),)),
            ],
            compiler_params=pltpu.CompilerParams(collective_id=0, has_side_effects=True),
            name="flame",
        )(density, momentum, hydrogen, modes, jnp.asarray(early), jnp.asarray(back), jnp.asarray(late))
        return tuple(pl.pallas_call(
            write_out,
            out_shape=[jax.ShapeDtypeStruct(local, f32)] * 3,
            in_specs=[pl.BlockSpec(memory_space=pltpu.VMEM)] * 3,
            out_specs=[any_spec] * 3,
            scratch_shapes=[pltpu.SemaphoreType.DMA((3,))],
            name="write",
        )(*[pltpu.with_memory_space_constraint(r, pltpu.VMEM) for r in rates]))

    in_specs = (P("gx", "gy", "gz"), P("gx", "gy", "gz"), P("gx", "gy", "gz"), P())
    out_specs = (P("gx", "gy", "gz"), P("gx", "gy", "gz"), P("gx", "gy", "gz"))
    return jax.shard_map(
        per_device, mesh=mesh, in_specs=in_specs, out_specs=out_specs, check_vma=False
    )
```
